32 devices in a mesh: items: 4 (over y, x), seq: 8 (over z, core).
Axes of the slice: x: 2, y: 2, z: 4, core: 2. Of those that a mesh axis runs over, the one named last changes fastest.
Arguments:
- byte_tokens: int32 [4, 4096], P('items', 'seq'), may hold values from 0 to 255
- groups: int32 [4, 4096], P('items', 'seq'), may hold values from 0 to 3, as said below
- doc_ids: int32 [4, 512], P('items'), may hold values from 0 to 7, never falling along the last dimension, each value on 1 to 256 neighbouring positions
- patch_proj: float32 [6144, 768], P(('items', 'seq')), may hold values from -0.078125 to 0.078125
- tables: float32 [3, 256, 768], P(None, ('items', 'seq'))
- attn_qkv: float32 [2, 768, 2304], P(None, ('items', 'seq')), may hold values from -0.21875 to 0.21875
- attn_out: float32 [2, 768, 768], P(None, ('items', 'seq')), may hold values from -0.625 to 0.625
- mlp_in: float32 [2, 768, 3072], P(None, ('items', 'seq')), may hold values from -0.21875 to 0.21875
- mlp_out: float32 [2, 3072, 768], P(None, ('items', 'seq')), may hold values from -0.109375 to 0.109375
- vectors: float32 [14, 768], replicated
- first_proj: float32 [6144, 768], P(('items', 'seq')), may hold values from -1.4305115e-06 to 1.4305115e-06
- first_tables: float32 [3, 256, 768], P(None, ('items', 'seq')), may hold values from -1.4305115e-06 to 1.4305115e-06
- first_qkv: float32 [2, 768, 2304], P(None, ('items', 'seq')), may hold values from -1.4305115e-06 to 1.4305115e-06
- first_out: float32 [2, 768, 768], P(None, ('items', 'seq')), may hold values from -1.4305115e-06 to 1.4305115e-06
- first_in: float32 [2, 768, 3072], P(None, ('items', 'seq')), may hold values from -1.4305115e-06 to 1.4305115e-06
- first_down: float32 [2, 3072, 768], P(None, ('items', 'seq')), may hold values from -1.4305115e-06 to 1.4305115e-06
- first_vectors: float32 [14, 768], replicated, may hold values from -7.6293945e-06 to 7.6293945e-06
- second_proj: float32 [6144, 768], P(('items', 'seq')), may hold values from 2.7214456e-13 to 1.0783087e-12
- second_tables: float32 [3, 256, 768], P(None, ('items', 'seq')), may hold values from 2.7214456e-13 to 1.0783087e-12
- second_qkv: float32 [2, 768, 2304], P(None, ('items', 'seq')), may hold values from 2.7214456e-13 to 1.0783087e-12
- second_out: float32 [2, 768, 768], P(None, ('items', 'seq')), may hold values from 2.7214456e-13 to 1.0783087e-12
- second_in: float32 [2, 768, 3072], P(None, ('items', 'seq')), may hold values from 2.7214456e-13 to 1.0783087e-12
- second_down: float32 [2, 3072, 768], P(None, ('items', 'seq')), may hold values from 2.7214456e-13 to 1.0783087e-12
- second_vectors: float32 [14, 768], replicated, may hold values from 6.6752437e-12 to 2.7214456e-11
Outputs:
- loss: float32 [], replicated
- grad_norm: float32 [], replicated
- new_proj: float32 [6144, 768], P(('items', 'seq'))
- new_tables: float32 [3, 256, 768], P(None, ('items', 'seq'))
- new_qkv: float32 [2, 768, 2304], P(None, ('items', 'seq'))
- new_out: float32 [2, 768, 768], P(None, ('items', 'seq'))
- new_in: float32 [2, 768, 3072], P(None, ('items', 'seq'))
- new_down: float32 [2, 3072, 768], P(None, ('items', 'seq'))
- new_vectors: float32 [14, 768], replicated
- moment_proj: float32 [6144, 768], P(('items', 'seq'))
- moment_tables: float32 [3, 256, 768], P(None, ('items', 'seq'))
- moment_qkv: float32 [2, 768, 2304], P(None, ('items', 'seq'))
- moment_out: float32 [2, 768, 768], P(None, ('items', 'seq'))
- moment_in: float32 [2, 768, 3072], P(None, ('items', 'seq'))
- moment_down: float32 [2, 3072, 768], P(None, ('items', 'seq'))
- moment_vectors: float32 [14, 768], replicated
- square_proj: float32 [6144, 768], P(('items', 'seq'))
- square_tables: float32 [3, 256, 768], P(None, ('items', 'seq'))
- square_qkv: float32 [2, 768, 2304], P(None, ('items', 'seq'))
- square_out: float32 [2, 768, 768], P(None, ('items', 'seq'))
- square_in: float32 [2, 768, 3072], P(None, ('items', 'seq'))
- square_down: float32 [2, 3072, 768], P(None, ('items', 'seq'))
- square_vectors: float32 [14, 768], replicated
The draws below stay inside these ranges and needn't reach their ends.
Inputs may be any that keep to these rules, and one draw needn't show every extreme that they name: `groups`: every item holds each group id at least once.
All inputs are finite; a program needn't handle non-finite values.
Results may differ from the reference program's by a relative error of at most 0.0089.
Values may be sent and summed in bfloat16 or wider, within the bound.
No kernel may reach another device: no remote copies, remote signals or barrier semaphores. Data moves between devices by JAX's collectives and lax.ppermute only.
A program may use at most 256 MiB of HBM per device.

```python
import math
import jax
import jax.numpy as jnp
import numpy as np
from jax import lax

D = 768
HEADS = 12
HEAD_DIM = 64
FF = 3072
PATCH = 8
VOCAB = 256
GROUPS = 4
DOCS = 8
STEP_NUMBER = 7
ITEMS = 4
PATCHES = 512
BYTES = 4096
DOC_MOST = 256
VEC_ROWS = 14
PARAMS = 19474944


def draw_groups(key, part):
    raw = jax.random.randint(key, (ITEMS, BYTES), 0, GROUPS)
    place = jnp.broadcast_to(jnp.arange(BYTES)[None, :], (ITEMS, BYTES))
    return jnp.where(place < GROUPS, place, raw).astype(jnp.int32)


def draw_tables(key, part):
    noise = jax.random.normal(key, (3, VOCAB, D), jnp.float32)
    scale = jnp.where(jnp.arange(3) == 2, 2.0 / D ** 0.5, 1.0)[:, None, None]
    return noise * scale


def draw_vectors(key, part):
    noise = jax.random.normal(key, (VEC_ROWS, D), jnp.float32)
    rows = jnp.arange(VEC_ROWS)[:, None]
    return jnp.where(rows < 5, 1.0 + 0.1 * noise, noise)


def touch_ends(values, stream_key, smallest, high):
    spot = [jax.random.randint(jax.random.fold_in(stream_key, axis), (), 0, length) for axis, length in enumerate(values.shape)]
    main_axis = values.shape.index(max(values.shape))
    beside = spot[:main_axis] + [(spot[main_axis] + 1) % values.shape[main_axis]] + spot[main_axis + 1:]
    return values.at[tuple(spot)].set(smallest).at[tuple(beside)].set(high)


def shard_levels(key, shape, shards, low, top_value):
    level = 1.0
    for axis_at, parts in shards:
        steps = jax.random.uniform(jax.random.fold_in(jax.random.fold_in(key, 6), axis_at), (parts,), jnp.float32, low / len(shards), top_value / len(shards))
        level = level * jnp.repeat(jnp.exp(steps), shape[axis_at] // parts).reshape((-1,) + (1,) * (len(shape) - 1 - axis_at))
    return level


def cumulative_ranks(count, skew):
    weights = [(1 << 20) // math.isqrt(standing ** skew) + 1 for standing in range(1, count + 1)]
    deviation = 1 + sum(weights) // (1 << 30)
    return np.cumsum(np.array([max(1, weight // deviation) for weight in weights]))


def ranked_ids(stream_key, extent, number_of, slope):
    table = cumulative_ranks(number_of, slope)
    lot = jax.random.randint(jax.random.fold_in(stream_key, 1), extent, 0, int(table[number_of - 1]))
    standing = jnp.searchsorted(jnp.asarray(table, jnp.int32), lot, side="right")
    return jax.random.permutation(jax.random.fold_in(stream_key, 2), number_of)[standing].astype(jnp.int32)


def length_profile(count, total, most, slope):
    weights = [(1 << 20) // math.isqrt(rank ** slope) + 1 for rank in range(2, count + 1)]
    spare, given = total - most - (count - 1), [1] * (count - 1)
    while spare > 0:
        movable = [i for i in range(count - 1) if given[i] < most]
        mass, left = sum([weights[i] for i in movable]), spare
        for i in movable:
            extra = min(most - given[i], max(1, left * weights[i] // mass), spare)
            given[i] = given[i] + extra
            spare = spare - extra
    return np.array([most] + given)


def ragged(key, number_of, total, reach, lean):
    if number_of == 2:
        one = jax.random.randint(key, (), max(1, total - reach), min(reach, total - 1) + 1)
        return jnp.stack([one, total - one])
    tallies = jnp.asarray(length_profile(number_of, total, reach, lean), jnp.int32)
    couples = (number_of - 1) // 2
    giver, sink = tallies[1:1 + 2 * couples:2], tallies[2:2 + 2 * couples:2]
    slack = jnp.minimum(giver - 1, reach - sink)
    shifted = jax.random.randint(jax.random.fold_in(key, 1), (couples,), 0, 1 << 20) % (slack + 1)
    tallies = tallies.at[1:1 + 2 * couples:2].set(giver - shifted).at[2:2 + 2 * couples:2].set(sink + shifted)
    return tallies[jax.random.permutation(jax.random.fold_in(key, 2), number_of)]


def centred(key, shape, deviation, reach, cuts=(), kind=jnp.bfloat16):
    drawn = jax.random.normal(key, shape, jnp.float32) * deviation
    if len(cuts) > 0:
        drawn = shard_levels(key, shape, cuts, -0.22, 0.18) * drawn
    return jnp.clip(drawn, min=-reach, max=reach).astype(kind)


def setup_inputs(seed: int = 0) -> dict:
    key_list = jax.random.split(jax.random.key(seed), 25)
    return {
        "byte_tokens": touch_ends(ranked_ids(key_list[0], (ITEMS, BYTES), VOCAB, 1), jax.random.fold_in(key_list[0], 3), 0, VOCAB - 1).astype(jnp.int32),
        "groups": draw_groups(jax.random.fold_in(key_list[24], 71), 0),
        "doc_ids": jax.vmap(lambda own: jnp.searchsorted(jnp.cumsum(ragged(own, DOCS, PATCHES, DOC_MOST, 1)), jnp.arange(PATCHES), side="right"))(jax.random.split(key_list[2], ITEMS)).reshape((ITEMS, PATCHES)).astype(jnp.int32),
        "patch_proj": centred(key_list[3], (PATCH * D, D), (PATCH * D) ** -0.5, 0.078125, ((0, 32),), jnp.float32),
        "tables": draw_tables(jax.random.fold_in(key_list[24], 71), 0),
        "attn_qkv": centred(key_list[5], (2, D, 3 * D), D ** -0.5, 0.21875, ((1, 32),), jnp.float32),
        "attn_out": centred(key_list[6], (2, D, D), (D // 8) ** -0.5, 0.625, ((1, 32),), jnp.float32),
        "mlp_in": centred(key_list[7], (2, D, FF), D ** -0.5, 0.21875, ((1, 32),), jnp.float32),
        "mlp_out": centred(key_list[8], (2, FF, D), FF ** -0.5, 0.109375, ((1, 32),), jnp.float32),
        "vectors": draw_vectors(jax.random.fold_in(key_list[24], 71), 0),
        "first_proj": centred(key_list[10], (PATCH * D, D), (0.0011 * PARAMS ** -0.5), 1.430511474609375e-06, ((0, 32),), jnp.float32),
        "first_tables": centred(key_list[11], (3, VOCAB, D), (0.0011 * PARAMS ** -0.5), 1.430511474609375e-06, ((1, 32),), jnp.float32),
        "first_qkv": centred(key_list[12], (2, D, 3 * D), (0.0011 * PARAMS ** -0.5), 1.430511474609375e-06, ((1, 32),), jnp.float32),
        "first_out": centred(key_list[13], (2, D, D), (0.0011 * PARAMS ** -0.5), 1.430511474609375e-06, ((1, 32),), jnp.float32),
        "first_in": centred(key_list[14], (2, D, FF), (0.0011 * PARAMS ** -0.5), 1.430511474609375e-06, ((1, 32),), jnp.float32),
        "first_down": centred(key_list[15], (2, FF, D), (0.0011 * PARAMS ** -0.5), 1.430511474609375e-06, ((1, 32),), jnp.float32),
        "first_vectors": centred(key_list[16], (VEC_ROWS, D), (0.0055 * PARAMS ** -0.5), 7.62939453125e-06, (), jnp.float32),
        "second_proj": jnp.clip(jnp.exp(math.log(1.0783086663163077e-12) - 1.3768157 * jax.random.uniform(key_list[17], (PATCH * D, D), jnp.float32) ** shard_levels(key_list[17], (PATCH * D, D), ((0, 32),), -0.2, 0.2)), 2.721445573235226e-13, 1.0783086663163077e-12),
        "second_tables": jnp.clip(jnp.exp(math.log(1.0783086663163077e-12) - 1.3768157 * jax.random.uniform(key_list[18], (3, VOCAB, D), jnp.float32) ** shard_levels(key_list[18], (3, VOCAB, D), ((1, 32),), -0.2, 0.2)), 2.721445573235226e-13, 1.0783086663163077e-12),
        "second_qkv": jnp.clip(jnp.exp(math.log(1.0783086663163077e-12) - 1.3768157 * jax.random.uniform(key_list[19], (2, D, 3 * D), jnp.float32) ** shard_levels(key_list[19], (2, D, 3 * D), ((1, 32),), -0.2, 0.2)), 2.721445573235226e-13, 1.0783086663163077e-12),
        "second_out": jnp.clip(jnp.exp(math.log(1.0783086663163077e-12) - 1.3768157 * jax.random.uniform(key_list[20], (2, D, D), jnp.float32) ** shard_levels(key_list[20], (2, D, D), ((1, 32),), -0.2, 0.2)), 2.721445573235226e-13, 1.0783086663163077e-12),
        "second_in": jnp.clip(jnp.exp(math.log(1.0783086663163077e-12) - 1.3768157 * jax.random.uniform(key_list[21], (2, D, FF), jnp.float32) ** shard_levels(key_list[21], (2, D, FF), ((1, 32),), -0.2, 0.2)), 2.721445573235226e-13, 1.0783086663163077e-12),
        "second_down": jnp.clip(jnp.exp(math.log(1.0783086663163077e-12) - 1.3768157 * jax.random.uniform(key_list[22], (2, FF, D), jnp.float32) ** shard_levels(key_list[22], (2, FF, D), ((1, 32),), -0.2, 0.2)), 2.721445573235226e-13, 1.0783086663163077e-12),
        "second_vectors": jnp.clip(jnp.exp(jax.random.uniform(key_list[23], (VEC_ROWS, D), jnp.float32, math.log(6.675243691134369e-12), math.log(2.7214456382873564e-11))), 6.675243691134369e-12, 2.7214456382873564e-11),
    }


@jax.custom_vjp
def low(v):
    return lax.optimization_barrier(v.astype(jnp.bfloat16)).astype(jnp.float32)

@jax.custom_vjp
def low_back(v):
    return v

def low_keep(v):
    return (low(v), None)

def low_pass(kept, grad):
    return (grad,)

def back_keep(v):
    return (v, None)

def back_low(kept, grad):
    return (low(grad),)
low.defvjp(low_keep, low_pass)
low_back.defvjp(back_keep, back_low)
EPSILON = 1e-05
CLIP_AT = 0.01
BETA_ONE = 0.9
BETA_TWO = 0.95
ADAM_EPS = 1e-08
DECAY = 0.1
NEGATIVE = -1e+30
HIGH = lax.Precision.HIGHEST

def matmul(left, right):
    return low_back(jnp.dot(low(left), right, precision=HIGH))

def rms_norm(values, gain):
    return values * lax.rsqrt(lax.optimization_barrier(jnp.mean(values * values, axis=-1, keepdims=True)) + EPSILON) * gain

def global_attend(queries, keys, values, docs):
    queries = queries.reshape(PATCHES, HEADS, HEAD_DIM)
    keys = keys.reshape(PATCHES, HEADS, HEAD_DIM)
    values = values.reshape(PATCHES, HEADS, HEAD_DIM)
    block = min(512, PATCHES)
    positions = jnp.arange(PATCHES).astype(jnp.int32)

    def one_block(begin):
        rows = lax.dynamic_slice_in_dim(queries, begin, block, 0)
        row_pos = begin + jnp.arange(block).astype(jnp.int32)
        row_docs = lax.dynamic_slice_in_dim(docs, begin, block, 0)
        scores = low_back(jnp.einsum('qhd,khd->hqk', rows, keys, precision=HIGH) * HEAD_DIM ** (-0.5))
        allowed = (positions[None, :] <= row_pos[:, None]) & (docs[None, :] == row_docs[:, None])
        probs = jax.nn.softmax(jnp.where(allowed[None], scores, NEGATIVE), axis=-1)
        return jnp.einsum('hqk,khd->qhd', low(probs), values, precision=HIGH)
    starts = (jnp.arange(PATCHES // block) * block).astype(jnp.int32)
    mixed = lax.map(jax.checkpoint(one_block), starts)
    return mixed.reshape(PATCHES, D)

def local_attend(queries, keys, values):
    shape = (BYTES // PATCH, PATCH, HEADS, HEAD_DIM)
    queries, keys, values = (queries.reshape(shape), keys.reshape(shape), values.reshape(shape))
    scores = low_back(jnp.einsum('pqhd,pkhd->phqk', queries, keys, precision=HIGH) * HEAD_DIM ** (-0.5))
    causal = jnp.tril(jnp.ones((PATCH, PATCH), bool))
    probs = jax.nn.softmax(jnp.where(causal, scores, NEGATIVE), axis=-1)
    mixed = jnp.einsum('phqk,pkhd->pqhd', low(probs), values, precision=HIGH)
    return mixed.reshape(BYTES, D)

def layer(resid, gains, w_qkv, w_out, w_in, w_down, attend):
    qkv = low(matmul(rms_norm(resid, gains[0]), w_qkv))
    mixed = low_back(attend(qkv[:, :D], qkv[:, D:2 * D], qkv[:, 2 * D:]))
    resid = resid + matmul(mixed, w_out)
    hidden = matmul(rms_norm(resid, gains[1]), w_in)
    return resid + matmul(jax.nn.gelu(hidden), w_down)

def item_terms(rounded, vectors, item_bytes, item_groups, item_docs):
    proj, tables, w_qkv, w_out, w_in, w_down = rounded
    byte_grid = item_bytes.reshape(PATCHES, PATCH)
    inputs = tables[0][byte_grid].reshape(PATCHES, PATCH * D)
    embedded = matmul(inputs, proj)
    previous = jnp.concatenate([jnp.zeros((1, D), embedded.dtype), embedded[:-1]], axis=0)
    starts = jnp.concatenate([jnp.ones((1,), bool), item_docs[1:] != item_docs[:-1]])
    resid = jnp.where(starts[:, None], vectors[5][None, :], previous)

    def global_mix(queries, keys, values):
        return global_attend(queries, keys, values, item_docs)
    top = layer(resid, vectors[0:2], w_qkv[0], w_out[0], w_in[0], w_down[0], global_mix)
    before = jnp.concatenate([jnp.zeros((PATCHES, 1), jnp.int32), byte_grid[:, :-1]], axis=1)
    keep_first = (jnp.arange(PATCH) > 0).astype(top.dtype)
    local_in = tables[1][before] * keep_first[None, :, None] + top[:, None, :] + vectors[6:6 + PATCH][None]
    result = layer(local_in.reshape(BYTES, D), vectors[2:4], w_qkv[1], w_out[1], w_in[1], w_down[1], local_attend)
    logits = matmul(rms_norm(result, vectors[4]), tables[2].T)
    lse = jax.nn.logsumexp(logits, axis=-1)
    target = jnp.take_along_axis(logits, item_bytes[:, None], axis=-1)[:, 0]
    group_hot = (item_groups[:, None] == jnp.arange(GROUPS)[None, :]).astype(logits.dtype)
    return lax.optimization_barrier(jnp.sum((lse - target)[:, None] * group_hot, axis=0))

def adam_step(weight, grad, first, second, rate, count):
    first = BETA_ONE * first + (1.0 - BETA_ONE) * grad
    second = BETA_TWO * second + (1.0 - BETA_TWO) * grad * grad
    first_hat = first / (1.0 - BETA_ONE ** count)
    second_hat = second / (1.0 - BETA_TWO ** count)
    return (weight - rate * (first_hat / (jnp.sqrt(second_hat) + ADAM_EPS) + DECAY * weight), first, second)

def reference(byte_tokens, groups, doc_ids, patch_proj, tables, attn_qkv, attn_out, mlp_in, mlp_out, vectors, first_proj, first_tables, first_qkv, first_out, first_in, first_down, first_vectors, second_proj, second_tables, second_qkv, second_out, second_in, second_down, second_vectors):
    masters = (patch_proj, tables, attn_qkv, attn_out, mlp_in, mlp_out, vectors)
    group_hot = (groups.reshape(-1)[:, None] == jnp.arange(GROUPS)[None, :]).astype(jnp.float32)
    counts = lax.optimization_barrier(jnp.sum(group_hot, axis=0))

    def loss_fn(params):
        rounded = tuple((low(piece) for piece in params[:6]))

        def scan_item(total, item):
            return (total + item_terms(rounded, params[6], item[0], item[1], item[2]), None)
        total, _ = lax.scan(scan_item, jnp.zeros((GROUPS,), jnp.float32), (byte_tokens, groups, doc_ids))
        return jnp.sum(total / counts) / GROUPS
    loss, pullback = jax.vjp(loss_fn, masters)
    grads = pullback(jnp.ones_like(loss))[0]
    grad_norm = jnp.sqrt(sum((jnp.sum(piece * piece) for piece in grads)))
    factor = jnp.minimum(1.0, CLIP_AT / grad_norm)
    count = float(STEP_NUMBER)
    rates = ((PATCH * D) ** (-0.5), jnp.array([1.0, 1.0, 2.0 * D ** (-0.5)], jnp.float32).reshape(3, 1, 1), D ** (-0.5), (D // 8) ** (-0.5), D ** (-0.5), FF ** (-0.5), 0.5)
    firsts = (first_proj, first_tables, first_qkv, first_out, first_in, first_down, first_vectors)
    seconds = (second_proj, second_tables, second_qkv, second_out, second_in, second_down, second_vectors)
    done = [adam_step(masters[n], grads[n] * factor, firsts[n], seconds[n], rates[n], count) for n in range(7)]
    return (loss, grad_norm, done[0][0], done[1][0], done[2][0], done[3][0], done[4][0], done[5][0], done[6][0], done[0][1], done[1][1], done[2][1], done[3][1], done[4][1], done[5][1], done[6][1], done[0][2], done[1][2], done[2][2], done[3][2], done[4][2], done[5][2], done[6][2])
```

```python
import jax
import jax.numpy as jnp
from jax import lax
from jax.sharding import PartitionSpec as P

D = 768
HEAD_DIM = 64
FF = 3072
PATCH = 8
VOCAB = 256
GROUPS = 4
STEP_NUMBER = 7


EPSILON = 1e-05
CLIP_AT = 0.01
BETA_ONE = 0.9
BETA_TWO = 0.95
ADAM_EPS = 1e-08
DECAY = 0.1
NEGATIVE = -1e30
HIGH = lax.Precision.HIGHEST


def from_behind(value, axis, steps):
    count = lax.axis_size(axis)
    first, last = (max(0, -steps), min(count, count - steps))
    return lax.ppermute(value, axis, [(source, source + steps) for source in range(first, last)])


def norm_forward(values, gain):
    scale = lax.rsqrt(jnp.mean(values * values, axis=-1, keepdims=True) + EPSILON)
    normed = values * scale
    return (normed * gain, (normed, scale))


def norm_backward(upstream, normed, scale, gain):
    gain_grad = jnp.sum(upstream * normed, axis=0)
    inner = upstream * gain
    return (scale * (inner - normed * jnp.mean(inner * normed, axis=-1, keepdims=True)), gain_grad)


def to_half(value):
    return value.astype(jnp.bfloat16)


def wide(value):
    return value.astype(jnp.float32)


def pick(value, index, axis):
    return lax.dynamic_index_in_dim(value, index, axis, keepdims=False)


def swap(value, axis, bit):
    count = lax.axis_size(axis)
    return lax.ppermute(value, axis, [(at, at ^ bit) for at in range(count)])


def fold(value, axis, bit, mine, place):
    got = swap(to_half(pick(value, 1 - mine, place)), axis, bit)
    return wide(pick(value, mine, place)) + wide(got)


def reduce_rows(partial, x_first):
    items, seq = lax.axis_size("items"), lax.axis_size("seq")
    at_item, at_seq = lax.axis_index("items"), lax.axis_index("seq")
    core, x_at, y_at = at_seq % 2, at_item % 2, at_item // 2
    width = partial.shape[1]
    grid = partial.reshape(items // 2, 2, seq // 2, 2, -1, width)
    grid = fold(grid, "seq", 1, core, 3)
    if x_first:
        grid = fold(fold(grid, "items", 1, x_at, 1), "items", 2, y_at, 0)
    else:
        grid = fold(fold(grid, "items", 2, y_at, 0), "items", 1, x_at, 0)
    groups = [list(range(first, seq, 2)) for first in range(2)]
    pieces = lax.all_to_all(to_half(grid), "seq", 0, 0, axis_index_groups=groups, tiled=True)
    return jnp.sum(wide(pieces), axis=0)


def share(row):
    count = lax.axis_size("items") * lax.axis_size("seq")
    return lax.all_to_all(
        jnp.broadcast_to(row[None], (count,) + row.shape), ("items", "seq"), 0, 0, tiled=True
    )


def spread_sum(value):
    count = lax.axis_size("items") * lax.axis_size("seq")
    size = -(-value.shape[0] // count)
    rows = jnp.pad(value, (0, size * count - value.shape[0])).reshape(count, size)
    return jnp.sum(lax.all_to_all(rows, ("items", "seq"), 0, 0, tiled=True), axis=0)


def gather_rows(value):
    return lax.all_gather(value, ("items", "seq"), axis=0, tiled=True)


def one_hot(indices, width, dtype):
    return (indices.reshape(-1)[:, None] == jnp.arange(width)[None, :]).astype(dtype)


def layer_forward(resid, gains, qkv_w, out_w, in_w, down_w, attend):
    attn_in, (normed_one, scale_one) = norm_forward(resid, gains[0])
    attn_half = attn_in.astype(jnp.bfloat16)
    qkv_half = jnp.dot(attn_half, qkv_w, preferred_element_type=jnp.float32).astype(jnp.bfloat16)
    mixed, kept = attend(qkv_half)
    mixed_half = mixed.astype(jnp.bfloat16)
    middle = resid + jnp.dot(mixed_half, out_w, preferred_element_type=jnp.float32)
    mlp_norm, (normed_two, scale_two) = norm_forward(middle, gains[1])
    mlp_half = mlp_norm.astype(jnp.bfloat16)
    hidden = jnp.dot(mlp_half, in_w, preferred_element_type=jnp.float32)
    active_half = jax.nn.gelu(hidden).astype(jnp.bfloat16)
    result = middle + jnp.dot(active_half, down_w, preferred_element_type=jnp.float32)
    saved = (
        normed_one,
        scale_one,
        attn_half,
        qkv_half,
        mixed,
        mixed_half,
        kept,
        normed_two,
        scale_two,
        mlp_half,
        hidden,
        active_half,
    )
    return (result, saved)


def layer_backward(result_grad, saved, gains, qkv_w, out_w, in_w, down_w, attend_back):
    (
        normed_one,
        scale_one,
        attn_half,
        qkv_half,
        mixed,
        mixed_half,
        kept,
        normed_two,
        scale_two,
        mlp_half,
        hidden,
        active_half,
    ) = saved
    branch_half = result_grad.astype(jnp.bfloat16)
    down_grad = jnp.einsum(
        "rf,rd->fd", active_half, branch_half, preferred_element_type=jnp.float32
    )
    active_grad = jnp.einsum("rd,fd->rf", branch_half, down_w, preferred_element_type=jnp.float32)
    _, gelu_back = jax.vjp(jax.nn.gelu, hidden)
    hidden_half = gelu_back(active_grad)[0].astype(jnp.bfloat16)
    in_grad = jnp.einsum("rd,rf->df", mlp_half, hidden_half, preferred_element_type=jnp.float32)
    mlp_grad = jnp.einsum("rf,df->rd", hidden_half, in_w, preferred_element_type=jnp.float32)
    middle_grad, gain_two = norm_backward(mlp_grad, normed_two, scale_two, gains[1])
    middle_grad = middle_grad + result_grad
    proj_half = middle_grad.astype(jnp.bfloat16)
    out_grad = jnp.einsum("re,rd->ed", mixed_half, proj_half, preferred_element_type=jnp.float32)
    mixed_grad = jnp.einsum("rd,ed->re", proj_half, out_w, preferred_element_type=jnp.float32)
    qkv_grad_half = attend_back(mixed_grad.astype(jnp.bfloat16), qkv_half, kept, mixed).astype(
        jnp.bfloat16
    )
    qkv_grad = jnp.einsum("rd,re->de", attn_half, qkv_grad_half, preferred_element_type=jnp.float32)
    attn_grad = jnp.einsum("re,de->rd", qkv_grad_half, qkv_w, preferred_element_type=jnp.float32)
    resid_grad, gain_one = norm_backward(attn_grad, normed_one, scale_one, gains[0])
    attn_part = jnp.concatenate([to_half(qkv_grad), to_half(out_grad)], axis=1)
    return (
        resid_grad + middle_grad,
        (jnp.stack([gain_one, gain_two]), attn_part, to_half(in_grad), to_half(down_grad)),
    )


def local_forward(qkv_half):
    rows = qkv_half.shape[0]
    heads = qkv_half.shape[1] // (3 * HEAD_DIM)
    grid = qkv_half.reshape(rows // PATCH, PATCH, 3, heads, HEAD_DIM)
    scores = jnp.einsum(
        "pqhd,pkhd->phqk", grid[:, :, 0], grid[:, :, 1], preferred_element_type=jnp.float32
    ) * HEAD_DIM ** (-0.5)
    causal = jnp.tril(jnp.ones((PATCH, PATCH), bool))
    probs = jax.nn.softmax(jnp.where(causal, scores, NEGATIVE), axis=-1)
    mixed = jnp.einsum(
        "phqk,pkhd->pqhd",
        probs.astype(jnp.bfloat16),
        grid[:, :, 2],
        preferred_element_type=jnp.float32,
    )
    return (mixed.reshape(rows, heads * HEAD_DIM), probs)


def local_backward(grad_half, qkv_half, probs, mixed):
    rows = qkv_half.shape[0]
    heads = qkv_half.shape[1] // (3 * HEAD_DIM)
    grid = qkv_half.reshape(rows // PATCH, PATCH, 3, heads, HEAD_DIM)
    upstream = grad_half.reshape(rows // PATCH, PATCH, heads, HEAD_DIM)
    prob_grad = jnp.einsum(
        "pqhd,pkhd->phqk", upstream, grid[:, :, 2], preferred_element_type=jnp.float32
    )
    score_half = (probs * (prob_grad - jnp.sum(prob_grad * probs, axis=-1, keepdims=True))).astype(
        jnp.bfloat16
    )
    scale = HEAD_DIM ** (-0.5)
    query_grad = (
        jnp.einsum("phqk,pkhd->pqhd", score_half, grid[:, :, 1], preferred_element_type=jnp.float32)
        * scale
    )
    key_grad = (
        jnp.einsum("phqk,pqhd->pkhd", score_half, grid[:, :, 0], preferred_element_type=jnp.float32)
        * scale
    )
    value_grad = jnp.einsum(
        "phqk,pqhd->pkhd", probs.astype(jnp.bfloat16), upstream, preferred_element_type=jnp.float32
    )
    return jnp.stack([query_grad, key_grad, value_grad], axis=2).reshape(rows, 3 * heads * HEAD_DIM)


def adam_step(weight, grad, first, second, rate, count):
    first = BETA_ONE * first + (1.0 - BETA_ONE) * grad
    second = BETA_TWO * second + (1.0 - BETA_TWO) * grad * grad
    first_hat = first / (1.0 - BETA_ONE**count)
    second_hat = second / (1.0 - BETA_TWO**count)
    return (
        weight - rate * (first_hat / (jnp.sqrt(second_hat) + ADAM_EPS) + DECAY * weight),
        first,
        second,
    )


def body(
    byte_tokens,
    groups,
    doc_ids,
    patch_proj,
    tables,
    attn_qkv,
    attn_out,
    mlp_in,
    mlp_out,
    vectors,
    first_proj,
    first_tables,
    first_qkv,
    first_out,
    first_in,
    first_down,
    first_vectors,
    second_proj,
    second_tables,
    second_qkv,
    second_out,
    second_in,
    second_down,
    second_vectors,
):
    half = jnp.bfloat16
    single = jnp.float32
    width = vectors.shape[1]
    group_rows = share(groups.reshape(-1))
    counts = jnp.sum(one_hot(group_rows, GROUPS, single), axis=0)
    table_all = gather_rows(jnp.concatenate([tables[n].astype(half) for n in range(3)], axis=1))
    table_w = [table_all[:, n * width : (n + 1) * width] for n in range(3)]
    proj_w = gather_rows(patch_proj.astype(half))
    qkv_w, out_w, in_w, down_w = [], [], [], []
    for n in range(2):
        joined = gather_rows(
            jnp.concatenate(
                [attn_qkv[n].astype(half), attn_out[n].astype(half), mlp_in[n].astype(half)], axis=1
            )
        )
        qkv_w.append(joined[:, : 3 * width])
        out_w.append(joined[:, 3 * width : 4 * width])
        in_w.append(joined[:, 4 * width :])
        down_w.append(gather_rows(mlp_out[n].astype(half)))
    heads = width // HEAD_DIM
    scale = HEAD_DIM ** (-0.5)
    span_rows = byte_tokens.shape[1] // PATCH
    total_patches = doc_ids.shape[1]
    block = min(1024, total_patches)
    offset = lax.axis_index("seq") * span_rows
    my_pos = offset + jnp.arange(span_rows)
    keep_first = (jnp.arange(PATCH) > 0).astype(single)

    def key_slice(source, begin, length):
        return lax.dynamic_slice_in_dim(source, begin, length, 0)

    def scores_for(queries, query_pos, query_docs, key_block, key_pos, key_docs):
        scores = (
            jnp.einsum("qhd,khd->hqk", queries, key_block, preferred_element_type=single) * scale
        )
        allowed = (key_pos[None, :] <= query_pos[:, None]) & (
            key_docs[None, :] == query_docs[:, None]
        )
        return (scores, allowed[None])

    def over_keys(step_fn, carry):
        limit = total_patches // block
        return lax.fori_loop(0, limit, step_fn, carry)

    def item_pass(my_bytes, my_groups, all_docs):
        group_hot = one_hot(my_groups, GROUPS, single)
        my_docs = lax.dynamic_slice_in_dim(all_docs, offset, span_rows)
        prior_docs = jnp.concatenate(
            [lax.dynamic_slice_in_dim(all_docs, jnp.maximum(offset - 1, 0), 1), my_docs[:-1]]
        )
        starts = (my_pos == 0) | (my_docs != prior_docs)

        def block_at(queries, keys_all, values_all, number):
            begin = number * block
            key_block = key_slice(keys_all, begin, block)
            scores, allowed = scores_for(
                queries,
                my_pos,
                my_docs,
                key_block,
                begin + jnp.arange(block),
                key_slice(all_docs, begin, block),
            )
            return (scores, allowed, key_block, key_slice(values_all, begin, block))

        def global_forward(qkv_half):
            queries = qkv_half[:, :width].reshape(span_rows, heads, HEAD_DIM)
            keys_all, values_all = (
                lax.all_gather(qkv_half[:, width : 2 * width], "seq", axis=0, tiled=True),
                lax.all_gather(qkv_half[:, 2 * width :], "seq", axis=0, tiled=True),
            )
            keys_all = keys_all.reshape(total_patches, heads, HEAD_DIM)
            values_all = values_all.reshape(total_patches, heads, HEAD_DIM)

            def peak_step(number, carry):
                peak, total = carry
                scores, allowed, key_block, value_block = block_at(
                    queries, keys_all, values_all, number
                )
                masked = jnp.where(allowed, scores, NEGATIVE)
                new_peak = jnp.maximum(peak, jnp.max(masked, axis=-1))
                fresh = jnp.where(allowed, jnp.exp(masked - new_peak[..., None]), 0.0)
                return (new_peak, total * jnp.exp(peak - new_peak) + jnp.sum(fresh, axis=-1))

            begin_carry = (
                jnp.full((heads, span_rows), NEGATIVE, single),
                jnp.zeros((heads, span_rows), single),
            )
            peak, total = over_keys(peak_step, begin_carry)
            lse = peak + jnp.log(total)

            def mix_step(number, accum):
                scores, allowed, key_block, value_block = block_at(
                    queries, keys_all, values_all, number
                )
                probs = jnp.where(allowed, jnp.exp(scores - lse[..., None]), 0.0).astype(half)
                return accum + jnp.einsum(
                    "hqk,khd->qhd", probs, value_block, preferred_element_type=single
                )

            mixed = over_keys(mix_step, jnp.zeros((span_rows, heads, HEAD_DIM), single))
            return (mixed.reshape(span_rows, width), (queries, keys_all, values_all, lse))

        def global_backward(grad_half, qkv_half, kept, mixed):
            queries, keys_all, values_all, lse = kept
            upstream = grad_half.reshape(span_rows, heads, HEAD_DIM)
            delta = jnp.sum(
                upstream.astype(single) * mixed.reshape(span_rows, heads, HEAD_DIM), axis=-1
            ).T

            def query_step(number, accum):
                scores, allowed, key_block, value_block = block_at(
                    queries, keys_all, values_all, number
                )
                probs = jnp.where(allowed, jnp.exp(scores - lse[..., None]), 0.0)
                prob_grad = jnp.einsum(
                    "qhd,khd->hqk", upstream, value_block, preferred_element_type=single
                )
                score_half = (probs * (prob_grad - delta[..., None])).astype(half)
                return (
                    accum
                    + jnp.einsum(
                        "hqk,khd->qhd", score_half, key_block, preferred_element_type=single
                    )
                    * scale
                )

            query_grad = over_keys(query_step, jnp.zeros((span_rows, heads, HEAD_DIM), single))
            begin = jnp.int32(0)
            length = span_rows * lax.axis_size("seq")
            key_block = key_slice(keys_all, begin, length)
            value_block = key_slice(values_all, begin, length)
            scores, allowed = scores_for(
                queries,
                my_pos,
                my_docs,
                key_block,
                jnp.arange(length),
                key_slice(all_docs, begin, length),
            )
            probs = jnp.where(allowed, jnp.exp(scores - lse[..., None]), 0.0)
            prob_grad = jnp.einsum(
                "qhd,khd->hqk", upstream, value_block, preferred_element_type=single
            )
            score_half = (probs * (prob_grad - delta[..., None])).astype(half)
            value_grad = jnp.einsum(
                "hqk,qhd->khd", probs.astype(half), upstream, preferred_element_type=single
            )
            key_grad = (
                jnp.einsum("hqk,qhd->khd", score_half, queries, preferred_element_type=single)
                * scale
            )
            key_value_grad = lax.psum_scatter(
                jnp.concatenate(
                    [key_grad.reshape(length, width), value_grad.reshape(length, width)], axis=1
                ),
                "seq",
                scatter_dimension=0,
                tiled=True,
            )
            return jnp.concatenate([query_grad.reshape(span_rows, width), key_value_grad], axis=1)

        byte_grid = my_bytes.reshape(span_rows, PATCH)
        edge = from_behind(byte_grid[-1:], "seq", 1)
        earlier = jnp.concatenate([edge, byte_grid[:-1]], axis=0)
        earlier_hot = one_hot(earlier, VOCAB, half)
        embed_half = (
            jnp.dot(earlier_hot, table_w[0], preferred_element_type=single)
            .reshape(span_rows, PATCH * width)
            .astype(half)
        )
        projected = jnp.dot(embed_half, proj_w, preferred_element_type=single)
        resid = jnp.where(starts[:, None], vectors[5][None, :], projected)
        top, saved_top = layer_forward(
            resid, vectors[0:2], qkv_w[0], out_w[0], in_w[0], down_w[0], global_forward
        )
        before = jnp.concatenate([jnp.zeros((span_rows, 1), jnp.int32), byte_grid[:, :-1]], axis=1)
        before_hot = one_hot(before, VOCAB, half)
        local_embed = jnp.dot(before_hot, table_w[1], preferred_element_type=single).reshape(
            span_rows, PATCH, width
        )
        local_in = (
            local_embed * keep_first[None, :, None] + top[:, None, :] + vectors[6 : 6 + PATCH][None]
        )
        result, saved_low = layer_forward(
            local_in.reshape(span_rows * PATCH, width),
            vectors[2:4],
            qkv_w[1],
            out_w[1],
            in_w[1],
            down_w[1],
            local_forward,
        )
        final, (final_normed, final_scale) = norm_forward(result, vectors[4])
        final_half = final.astype(half)
        logits = jnp.einsum("rd,vd->rv", final_half, table_w[2], preferred_element_type=single)
        shifted = logits - jnp.max(logits, axis=-1, keepdims=True)
        totals = jnp.sum(jnp.exp(shifted), axis=-1, keepdims=True)
        probs = jnp.exp(shifted) / totals
        target_hot = one_hot(my_bytes, VOCAB, single)
        losses = jnp.log(totals[:, 0]) - jnp.sum(shifted * target_hot, axis=-1)
        loss_terms = jnp.sum(losses[:, None] * group_hot, axis=0)
        row_weight = jnp.sum(group_hot * (1.0 / (GROUPS * counts))[None, :], axis=-1)
        logit_half = (row_weight[:, None] * (probs - target_hot)).astype(half)
        head_grad = jnp.einsum("rv,rd->vd", logit_half, final_half, preferred_element_type=single)
        final_grad = jnp.einsum("rv,vd->rd", logit_half, table_w[2], preferred_element_type=single)
        result_grad, final_gain_grad = norm_backward(
            final_grad, final_normed, final_scale, vectors[4]
        )
        local_grad, low_grads = layer_backward(
            result_grad,
            saved_low,
            vectors[2:4],
            qkv_w[1],
            out_w[1],
            in_w[1],
            down_w[1],
            local_backward,
        )
        grid_grad = local_grad.reshape(span_rows, PATCH, width)
        top_grad = jnp.sum(grid_grad, axis=1)
        position_grad = jnp.sum(grid_grad, axis=0)
        masked_grad = (grid_grad * keep_first[None, :, None]).reshape(span_rows * PATCH, width)
        local_table_grad = jnp.einsum(
            "rv,rd->vd", before_hot.astype(single), masked_grad, precision=HIGH
        )
        resid_grad, top_grads = layer_backward(
            top_grad,
            saved_top,
            vectors[0:2],
            qkv_w[0],
            out_w[0],
            in_w[0],
            down_w[0],
            global_backward,
        )
        start_grad = jnp.sum(jnp.where(starts[:, None], resid_grad, 0.0), axis=0)
        projected_half = jnp.where(starts[:, None], 0.0, resid_grad).astype(half)
        proj_grad = jnp.einsum(
            "ri,rd->id", embed_half, projected_half, preferred_element_type=single
        )
        embed_grad = jnp.einsum("rd,id->ri", projected_half, proj_w, preferred_element_type=single)
        global_table_grad = jnp.einsum(
            "rv,rd->vd",
            earlier_hot.astype(single),
            embed_grad.reshape(span_rows * PATCH, width),
            precision=HIGH,
        )
        table_parts = jnp.concatenate(
            [to_half(global_table_grad), to_half(local_table_grad), to_half(head_grad)], axis=1
        )
        proj_rows = to_half(proj_grad)
        owned = (
            reduce_rows(low_grads[3], False),
            reduce_rows(low_grads[2], True),
            reduce_rows(low_grads[1], False),
            reduce_rows(top_grads[3], True),
            reduce_rows(top_grads[2], False),
            reduce_rows(top_grads[1], True),
            reduce_rows(proj_rows, False),
            reduce_rows(table_parts, True),
        )
        vector_grad = jnp.concatenate(
            [top_grads[0], low_grads[0], final_gain_grad[None], start_grad[None], position_grad],
            axis=0,
        )
        return (loss_terms, owned, vector_grad)

    loss_terms, pieces, vector_grad = item_pass(byte_tokens[0], groups[0], doc_ids[0])
    owned = (
        pieces[6],
        jnp.stack([pieces[7][:, n * width : (n + 1) * width] for n in range(3)]),
        jnp.stack([pieces[5][:, : 3 * width], pieces[2][:, : 3 * width]]),
        jnp.stack([pieces[5][:, 3 * width :], pieces[2][:, 3 * width :]]),
        jnp.stack([pieces[4], pieces[1]]),
        jnp.stack([pieces[3], pieces[0]]),
    )
    loss_total = jnp.sum(share(loss_terms), axis=0)
    vector_piece = spread_sum(vector_grad.reshape(-1))
    shard_square = sum((jnp.sum(piece * piece) for piece in owned))
    shard_square = shard_square + jnp.sum(vector_piece * vector_piece)
    tail = share(jnp.concatenate([vector_piece, shard_square[None]]))
    vector_total = tail[:, :-1].reshape(-1)[: vectors.size].reshape(vectors.shape)
    loss = jnp.sum(loss_total / counts) / GROUPS
    grad_norm = jnp.sqrt(jnp.sum(tail[:, -1]))
    factor = jnp.minimum(1.0, CLIP_AT / grad_norm)
    count = float(STEP_NUMBER)
    rates = (
        (PATCH * D) ** (-0.5),
        jnp.array([1.0, 1.0, 2.0 * D ** (-0.5)], single).reshape(3, 1, 1),
        D ** (-0.5),
        (D // 8) ** (-0.5),
        D ** (-0.5),
        FF ** (-0.5),
        0.5,
    )
    masters = (patch_proj, tables, attn_qkv, attn_out, mlp_in, mlp_out, vectors)
    grads = tuple(owned) + (vector_total,)
    firsts = (first_proj, first_tables, first_qkv, first_out, first_in, first_down, first_vectors)
    seconds = (
        second_proj,
        second_tables,
        second_qkv,
        second_out,
        second_in,
        second_down,
        second_vectors,
    )
    done = [
        adam_step(masters[n], grads[n] * factor, firsts[n], seconds[n], rates[n], count)
        for n in range(7)
    ]
    return (
        loss,
        grad_norm,
        done[0][0],
        done[1][0],
        done[2][0],
        done[3][0],
        done[4][0],
        done[5][0],
        done[6][0],
        done[0][1],
        done[1][1],
        done[2][1],
        done[3][1],
        done[4][1],
        done[5][1],
        done[6][1],
        done[0][2],
        done[1][2],
        done[2][2],
        done[3][2],
        done[4][2],
        done[5][2],
        done[6][2],
    )


def solution(mesh):
    return jax.shard_map(
        body,
        mesh=mesh,
        in_specs=(
            P("items", "seq"),
            P("items", "seq"),
            P("items", None),
            P(("items", "seq"), None),
            P(None, ("items", "seq"), None),
            P(None, ("items", "seq"), None),
            P(None, ("items", "seq"), None),
            P(None, ("items", "seq"), None),
            P(None, ("items", "seq"), None),
            P(),
            P(("items", "seq"), None),
            P(None, ("items", "seq"), None),
            P(None, ("items", "seq"), None),
            P(None, ("items", "seq"), None),
            P(None, ("items", "seq"), None),
            P(None, ("items", "seq"), None),
            P(),
            P(("items", "seq"), None),
            P(None, ("items", "seq"), None),
            P(None, ("items", "seq"), None),
            P(None, ("items", "seq"), None),
            P(None, ("items", "seq"), None),
            P(None, ("items", "seq"), None),
            P(),
        ),
        out_specs=(
            P(),
            P(),
            P(("items", "seq"), None),
            P(None, ("items", "seq"), None),
            P(None, ("items", "seq"), None),
            P(None, ("items", "seq"), None),
            P(None, ("items", "seq"), None),
            P(None, ("items", "seq"), None),
            P(),
            P(("items", "seq"), None),
            P(None, ("items", "seq"), None),
            P(None, ("items", "seq"), None),
            P(None, ("items", "seq"), None),
            P(None, ("items", "seq"), None),
            P(None, ("items", "seq"), None),
            P(),
            P(("items", "seq"), None),
            P(None, ("items", "seq"), None),
            P(None, ("items", "seq"), None),
            P(None, ("items", "seq"), None),
            P(None, ("items", "seq"), None),
            P(None, ("items", "seq"), None),
            P(),
        ),
        check_vma=False,
    )
```

```python
import jax
import jax.numpy as jnp
from jax import lax
from jax.experimental import pallas as pl
from jax.experimental.pallas import tpu as pltpu
from jax.sharding import PartitionSpec as P

D = 768
HEAD_DIM = 64
FF = 3072
PATCH = 8
VOCAB = 256
GROUPS = 4
STEP_NUMBER = 7


EPSILON = 1e-05
CLIP_AT = 0.01
BETA_ONE = 0.9
BETA_TWO = 0.95
ADAM_EPS = 1e-08
DECAY = 0.1
NEGATIVE = -1e30


def norm_forward(values, gain):
    scale = lax.rsqrt(jnp.mean(values * values, axis=-1, keepdims=True) + EPSILON)
    normed = values * scale
    return (normed * gain, (normed, scale))


def norm_backward(upstream, normed, scale, gain):
    gain_grad = jnp.sum(upstream * normed, axis=0)
    inner = upstream * gain
    return (scale * (inner - normed * jnp.mean(inner * normed, axis=-1, keepdims=True)), gain_grad)


def to_half(value):
    return value.astype(jnp.bfloat16)


def wide(value):
    return value.astype(jnp.float32)


def pick(value, index, axis):
    return lax.dynamic_index_in_dim(value, index, axis, keepdims=False)


def swap(value, axis, bit):
    count = lax.axis_size(axis)
    return lax.ppermute(value, axis, [(at, at ^ bit) for at in range(count)])


def same_core():
    seq = lax.axis_size("seq")
    return [list(range(first, seq, 2)) for first in range(2)]


def deal_depth(value):
    return lax.all_to_all(
        to_half(value), "seq", 0, 0, axis_index_groups=same_core(), tiled=True
    )


def along_depth(value):
    return jnp.sum(wide(deal_depth(value)), axis=0)


def gather_seq(value):
    seq = lax.axis_size("seq")
    mine = lax.all_to_all(
        jnp.broadcast_to(value[None], (seq // 2,) + value.shape),
        "seq",
        0,
        0,
        axis_index_groups=same_core(),
        tiled=True,
    )
    other = swap(mine, "seq", 1)
    second = lax.axis_index("seq") % 2 == 1
    pair = jnp.stack([jnp.where(second, other, mine), jnp.where(second, mine, other)], axis=1)
    return pair.reshape(seq * value.shape[0], value.shape[1])


def group_steps(partials, width, deal=True):
    items, seq = lax.axis_size("items"), lax.axis_size("seq")
    at_item, at_seq = lax.axis_index("items"), lax.axis_index("seq")
    core, x_at, y_at = at_seq % 2, at_item % 2, at_item // 2
    depth = seq // 2
    grids = [
        part.reshape(items // 2, 2, depth, 2, part.shape[0] // (items * seq), part.shape[1])
        for part in partials
    ]

    def side(index):
        return jnp.concatenate(
            [
                pick(grid, index, 3)[..., begin : begin + width]
                for grid in grids
                for begin in range(0, grid.shape[-1], width)
            ],
            axis=3,
        )

    kept = side(core)
    (sent,) = yield (side(1 - core),)
    (got,) = yield (swap(sent, "seq", 1),)
    rows = kept.shape[3]
    cut = rows // 16 * 8
    halves = ((0, cut), (cut, rows))

    def cells(value, y_from, y_count, x_from, x_count, half):
        begin, end = halves[half]
        return lax.dynamic_slice(
            value,
            (y_from, x_from, 0, begin, 0),
            (y_count, x_count, depth, end - begin, width),
        )

    def pair_sum(*where):
        return wide(cells(kept, *where)) + wide(cells(got, *where))

    to_x, to_y = yield (
        to_half(pair_sum(0, 2, 1 - x_at, 1, 0)),
        to_half(pair_sum(1 - y_at, 1, 0, 2, 1)),
    )
    first_in, second_in = yield swap(to_x, "items", 1), swap(to_y, "items", 2)
    to_y, to_x = yield (
        to_half(
            pair_sum(1 - y_at, 1, x_at, 1, 0)
            + wide(lax.dynamic_slice_in_dim(first_in, 1 - y_at, 1, 0))
        ),
        to_half(
            pair_sum(y_at, 1, 1 - x_at, 1, 1)
            + wide(lax.dynamic_slice_in_dim(second_in, 1 - x_at, 1, 1))
        ),
    )
    first_end, second_end = yield swap(to_y, "items", 2), swap(to_x, "items", 1)
    first = (
        pair_sum(y_at, 1, x_at, 1, 0)
        + wide(lax.dynamic_slice_in_dim(first_in, y_at, 1, 0))
        + wide(first_end)
    )
    second = (
        pair_sum(y_at, 1, x_at, 1, 1)
        + wide(lax.dynamic_slice_in_dim(second_in, x_at, 1, 1))
        + wide(second_end)
    )
    (blocks,) = yield (
        jnp.concatenate([to_half(first[0, 0]), to_half(second[0, 0])], axis=1),
    )
    if deal:
        (blocks,) = yield (deal_depth(blocks),)
    rows = jnp.sum(wide(blocks), axis=0)
    out, at = [], 0
    for grid in grids:
        deep, pieces = grid.shape[4], []
        for _ in range(0, grid.shape[-1], width):
            pieces.append(rows[at : at + deep])
            at += deep
        out.append(jnp.concatenate(pieces, axis=1))
    return out


def in_order(mine, other, bit, axis):
    return jnp.stack(
        [jnp.where(bit == 1, other, mine), jnp.where(bit == 1, mine, other)], axis=axis
    )


def gather_steps(mine):
    items, seq = lax.axis_size("items"), lax.axis_size("seq")
    at_item, at_seq = lax.axis_index("items"), lax.axis_index("seq")
    core, x_at, y_at = at_seq % 2, at_item % 2, at_item // 2
    rows, width = mine.shape[1:]
    cut = width // 2
    first, second = yield (mine[..., :cut], mine[..., cut:])
    to_x, to_y = yield (swap(first, "items", 1), swap(second, "items", 2))
    first, second = yield (in_order(first, to_x, x_at, 0), in_order(second, to_y, y_at, 0))
    to_y, to_x = yield (swap(first, "items", 2), swap(second, "items", 1))
    (mine,) = yield (
        jnp.concatenate(
            [in_order(first, to_y, y_at, 0), in_order(second, to_x, x_at, 1)], axis=-1
        ),
    )
    (other,) = yield (swap(mine, "seq", 1),)
    return in_order(mine, other, core, 3).reshape(items * seq * rows, width)


class Stepped:
    def __init__(self, steps):
        self.steps = steps
        self.held = next(self.steps)
        self.sending = True
        self.result = None

    def feed(self, arrays):
        try:
            self.held = self.steps.send(tuple(arrays))
        except StopIteration as end:
            self.held, self.result = (), end.value
        self.sending = not self.sending


def tie(values, groups):
    flat = list(values)
    for group in groups:
        flat.extend(group.held)
    flat = list(lax.optimization_barrier(tuple(flat)))
    values, flat = flat[: len(values)], flat[len(values) :]
    for group in groups:
        size = len(group.held)
        group.feed(flat[:size])
        flat = flat[size:]
    return values


def advance(values, *groups):
    waiting = [group for group in groups if group.result is None and not group.sending]
    if waiting:
        values = tie(values, waiting)
    sending = [group for group in groups if group.result is None]
    return tie(values, sending) if sending else values


def reduce_group(partials, width):
    group = Stepped(group_steps(partials, width))
    while group.result is None:
        advance([], group)
    return group.result


def share(row):
    count = lax.axis_size("items") * lax.axis_size("seq")
    return lax.all_to_all(
        jnp.broadcast_to(row[None], (count,) + row.shape), ("items", "seq"), 0, 0, tiled=True
    )


def spread(value):
    count = lax.axis_size("items") * lax.axis_size("seq")
    size = -(-value.shape[0] // count)
    return jnp.pad(value, (0, size * count - value.shape[0])).reshape(count, size)


def gather_rows(value):
    return lax.all_gather(value, ("items", "seq"), axis=0, tiled=True)


def one_hot(indices, width, dtype):
    return (indices.reshape(-1)[:, None] == jnp.arange(width)[None, :]).astype(dtype)


def hot_sum(hot, value):
    high = to_half(value)
    rest = to_half(value - wide(high))
    add = lambda term: jnp.einsum("rv,rd->vd", hot, term, preferred_element_type=jnp.float32)
    return add(high) + add(rest)


def layer_forward(resid, gains, qkv_w, out_w, in_w, down_w, attend):
    attn_in, (normed_one, scale_one) = norm_forward(resid, gains[0])
    attn_half = attn_in.astype(jnp.bfloat16)
    qkv_half = jnp.dot(attn_half, qkv_w, preferred_element_type=jnp.float32).astype(jnp.bfloat16)
    mixed, kept = attend(qkv_half)
    mixed_half = mixed.astype(jnp.bfloat16)
    middle = resid + jnp.dot(mixed_half, out_w, preferred_element_type=jnp.float32)
    mlp_norm, (normed_two, scale_two) = norm_forward(middle, gains[1])
    mlp_half = mlp_norm.astype(jnp.bfloat16)
    hidden = jnp.dot(mlp_half, in_w, preferred_element_type=jnp.float32)
    active_half = jax.nn.gelu(hidden).astype(jnp.bfloat16)
    result = middle + jnp.dot(active_half, down_w, preferred_element_type=jnp.float32)
    saved = (
        normed_one,
        scale_one,
        attn_half,
        qkv_half,
        mixed,
        mixed_half,
        kept,
        normed_two,
        scale_two,
        mlp_half,
        hidden,
        active_half,
    )
    return (result, saved)


def layer_backward(result_grad, saved, gains, qkv_w, out_w, in_w, down_w, attend_back, after):
    (
        normed_one,
        scale_one,
        attn_half,
        qkv_half,
        mixed,
        mixed_half,
        kept,
        normed_two,
        scale_two,
        mlp_half,
        hidden,
        active_half,
    ) = saved
    branch_half = result_grad.astype(jnp.bfloat16)
    active_grad = jnp.einsum("rd,fd->rf", branch_half, down_w, preferred_element_type=jnp.float32)
    _, gelu_back = jax.vjp(jax.nn.gelu, hidden)
    hidden_half = gelu_back(active_grad)[0].astype(jnp.bfloat16)
    hidden_half = after("mlp", hidden_half, (mlp_half, hidden_half), (active_half, branch_half))
    mlp_grad = jnp.einsum("rf,df->rd", hidden_half, in_w, preferred_element_type=jnp.float32)
    middle_grad, gain_two = norm_backward(mlp_grad, normed_two, scale_two, gains[1])
    middle_grad = middle_grad + result_grad
    proj_half = middle_grad.astype(jnp.bfloat16)
    mixed_grad = jnp.einsum("rd,ed->re", proj_half, out_w, preferred_element_type=jnp.float32)
    mixed_grad_half = after("attention", mixed_grad.astype(jnp.bfloat16))
    qkv_grad_half = attend_back(mixed_grad_half, qkv_half, kept, mixed).astype(jnp.bfloat16)
    qkv_grad_half = after("projections", qkv_grad_half, attn_half, mixed_half, proj_half)
    attn_grad = jnp.einsum("re,de->rd", qkv_grad_half, qkv_w, preferred_element_type=jnp.float32)
    resid_grad, gain_one = norm_backward(attn_grad, normed_one, scale_one, gains[0])
    resid_grad = after("end", resid_grad + middle_grad)
    return resid_grad, jnp.stack([gain_one, gain_two])


def outer(pair):
    return jnp.einsum("ri,rj->ij", *pair, preferred_element_type=jnp.float32)


def deal_columns(parts):
    count = lax.axis_size("items") * lax.axis_size("seq")
    rows = parts[0].shape[0]
    blocks = jnp.concatenate([part.reshape(rows, count, -1) for part in parts], axis=2)
    dealt = lax.all_to_all(
        blocks.transpose(1, 0, 2), ("items", "seq"), 0, 0, tiled=True
    ).reshape(count * rows, -1)
    out, at = [], 0
    for part in parts:
        size = part.shape[1] // count
        out.append(dealt[:, at : at + size])
        at += size
    return out


def deal_rows(parts):
    count = lax.axis_size("items") * lax.axis_size("seq")
    blocks = jnp.concatenate([to_half(part) for part in parts], axis=1)
    dealt = lax.all_to_all(
        blocks.reshape(count, -1, blocks.shape[1]), ("items", "seq"), 0, 0, tiled=True
    )
    out, at = [], 0
    for part in parts:
        size = part.shape[1]
        piece = dealt[:, :, at : at + size].transpose(1, 0, 2)
        out.append(wide(piece.reshape(piece.shape[0], -1)))
        at += size
    return out


ROWS = 128
LANES = 128


def contract(left, right, left_dim, right_dim):
    return lax.dot_general(
        left, right, (((left_dim,), (right_dim,)), ((), ())), preferred_element_type=jnp.float32
    )


def local_masks():
    row = lax.broadcasted_iota(jnp.int32, (ROWS, ROWS), 0)
    column = lax.broadcasted_iota(jnp.int32, (ROWS, ROWS), 1)
    allowed = (row // PATCH == column // PATCH) & (column <= row)
    lane = lax.broadcasted_iota(jnp.int32, (ROWS, LANES), 1)
    lanes = [
        jnp.where(lane // HEAD_DIM == head, 1.0, 0.0).astype(jnp.bfloat16)
        for head in range(LANES // HEAD_DIM)
    ]
    return allowed, lanes


def local_probs(query, key, allowed):
    scores = contract(query, key, 1, 1) * HEAD_DIM ** (-0.5)
    scores = jnp.where(allowed, scores, NEGATIVE)
    raised = jnp.exp(scores - jnp.max(scores, axis=-1, keepdims=True))
    return raised / jnp.sum(raised, axis=-1, keepdims=True)


def local_forward_kernel(qkv_ref, mixed_ref):
    width = mixed_ref.shape[1]
    allowed, lanes = local_masks()
    for begin in range(0, width, LANES):
        query, key, value = (
            qkv_ref[:, part * width + begin : part * width + begin + LANES] for part in range(3)
        )
        mixed = jnp.zeros((ROWS, LANES), jnp.float32)
        for mask in lanes:
            probs = local_probs(query * mask, key, allowed).astype(jnp.bfloat16)
            mixed = mixed + contract(probs, value * mask, 1, 0)
        mixed_ref[:, begin : begin + LANES] = mixed.astype(jnp.bfloat16)


def local_backward_kernel(qkv_ref, grad_ref, out_ref):
    width = grad_ref.shape[1]
    allowed, lanes = local_masks()
    scale = HEAD_DIM ** (-0.5)
    for begin in range(0, width, LANES):
        query, key, value = (
            qkv_ref[:, part * width + begin : part * width + begin + LANES] for part in range(3)
        )
        upstream = grad_ref[:, begin : begin + LANES]
        sums = [jnp.zeros((ROWS, LANES), jnp.float32) for _ in range(3)]
        for mask in lanes:
            head_query, head_upstream = query * mask, upstream * mask
            probs = local_probs(head_query, key, allowed)
            prob_grad = contract(head_upstream, value, 1, 1)
            inner = jnp.sum(prob_grad * probs, axis=-1, keepdims=True)
            score_half = (probs * (prob_grad - inner)).astype(jnp.bfloat16)
            sums[0] = sums[0] + contract(score_half, key * mask, 1, 0)
            sums[1] = sums[1] + contract(score_half, head_query, 0, 0)
            sums[2] = sums[2] + contract(probs.astype(jnp.bfloat16), head_upstream, 0, 0)
        for part, factor in enumerate((scale, scale, 1.0)):
            at = part * width + begin
            out_ref[:, at : at + LANES] = (sums[part] * factor).astype(jnp.bfloat16)


def by_rows(kernel, out_width, *operands):
    rows = operands[0].shape[0]
    moved = sum(value.size for value in operands) * 2 + rows * out_width * 2
    return pl.pallas_call(
        kernel,
        grid=(rows // ROWS,),
        in_specs=[pl.BlockSpec((ROWS, value.shape[1]), lambda at: (at, 0)) for value in operands],
        out_specs=pl.BlockSpec((ROWS, out_width), lambda at: (at, 0)),
        out_shape=jax.ShapeDtypeStruct((rows, out_width), jnp.bfloat16),
        cost_estimate=pl.CostEstimate(
            flops=rows * ROWS * out_width * 8, bytes_accessed=moved, transcendentals=rows * ROWS
        ),
    )(*operands)


def local_forward(qkv_half):
    return by_rows(local_forward_kernel, qkv_half.shape[1] // 3, qkv_half), None


def local_backward(grad_half, qkv_half, kept, mixed):
    return by_rows(local_backward_kernel, qkv_half.shape[1], qkv_half, grad_half)


def patch_probs(query, key, bias):
    scores = contract(query, key, 1, 1) * HEAD_DIM ** (-0.5) + bias
    raised = jnp.exp(scores - jnp.max(scores, axis=-1, keepdims=True))
    return raised / jnp.sum(raised, axis=-1, keepdims=True)


def head_lanes():
    lane = lax.broadcasted_iota(jnp.int32, (1, LANES), 1)
    return [
        jnp.where(lane // HEAD_DIM == head, 1.0, 0.0).astype(jnp.bfloat16)
        for head in range(LANES // HEAD_DIM)
    ]


def patch_forward_kernel(query_ref, key_ref, value_ref, bias_ref, mixed_ref):
    mixed = jnp.zeros(mixed_ref.shape, jnp.float32)
    for mask in head_lanes():
        probs = patch_probs(query_ref[...] * mask, key_ref[...], bias_ref[...])
        mixed = mixed + contract(probs.astype(jnp.bfloat16), value_ref[...] * mask, 1, 0)
    mixed_ref[...] = mixed.astype(jnp.bfloat16)


def patch_backward_kernel(query_ref, key_ref, value_ref, bias_ref, grad_ref, query_out, both_out):
    seq, _, span, _ = both_out.shape
    query_grad = jnp.zeros(query_out.shape, jnp.float32)
    key_grad = jnp.zeros(key_ref.shape, jnp.float32)
    value_grad = jnp.zeros(key_ref.shape, jnp.float32)
    for mask in head_lanes():
        query, upstream, key = query_ref[...] * mask, grad_ref[...] * mask, key_ref[...]
        probs = patch_probs(query, key, bias_ref[...])
        prob_grad = contract(upstream, value_ref[...], 1, 1)
        inner = jnp.sum(prob_grad * probs, axis=-1, keepdims=True)
        score_half = (probs * (prob_grad - inner)).astype(jnp.bfloat16)
        query_grad = query_grad + contract(score_half, key * mask, 1, 0)
        key_grad = key_grad + contract(score_half, query, 0, 0)
        value_grad = value_grad + contract(probs.astype(jnp.bfloat16), upstream, 0, 0)
    scale = HEAD_DIM ** (-0.5)
    query_out[...] = (query_grad * scale).astype(jnp.bfloat16)
    both_out[:, 0] = (key_grad * scale).astype(jnp.bfloat16).reshape(seq, span, LANES)
    both_out[:, 1] = value_grad.astype(jnp.bfloat16).reshape(seq, span, LANES)


def by_heads(kernel, out_shape, out_specs, qkv_half, both_all, bias, *others):
    rows, total, pairs = qkv_half.shape[0], both_all.shape[0], both_all.shape[1] // 2 // LANES
    columns = lambda count, shift: pl.BlockSpec((count, LANES), lambda at: (0, at + shift))
    return pl.pallas_call(
        kernel,
        grid=(pairs,),
        in_specs=[
            columns(rows, 0),
            columns(total, 0),
            columns(total, pairs),
            pl.BlockSpec((rows, total), lambda at: (0, 0)),
        ]
        + [columns(rows, 0) for _ in others],
        out_specs=out_specs,
        out_shape=out_shape,
    )(qkv_half, both_all, both_all, bias, *others)


def adam_step(weight, grad, first, second, rate, count):
    first = BETA_ONE * first + (1.0 - BETA_ONE) * grad
    second = BETA_TWO * second + (1.0 - BETA_TWO) * grad * grad
    first_hat = first / (1.0 - BETA_ONE**count)
    second_hat = second / (1.0 - BETA_TWO**count)
    return (
        weight - rate * (first_hat / (jnp.sqrt(second_hat) + ADAM_EPS) + DECAY * weight),
        first,
        second,
    )


def body(
    byte_tokens,
    groups,
    doc_ids,
    patch_proj,
    tables,
    attn_qkv,
    attn_out,
    mlp_in,
    mlp_out,
    vectors,
    first_proj,
    first_tables,
    first_qkv,
    first_out,
    first_in,
    first_down,
    first_vectors,
    second_proj,
    second_tables,
    second_qkv,
    second_out,
    second_in,
    second_down,
    second_vectors,
):
    half = jnp.bfloat16
    single = jnp.float32
    width = vectors.shape[1]
    depth = attn_qkv.shape[1]
    count = lax.axis_size("items") * lax.axis_size("seq")
    rank = lax.axis_index("items") * lax.axis_size("seq") + lax.axis_index("seq")
    told = share(jnp.concatenate([byte_tokens.reshape(-1), groups.reshape(-1)]))
    told = told.reshape(count, 2, -1)
    counts = jnp.sum(one_hot(told[:, 1], GROUPS, single), axis=0)

    def flat(value):
        return jnp.concatenate(
            [value[at : at + depth] for at in range(0, value.shape[0], depth)], axis=1
        ).astype(half)

    def tall(value):
        pieces = [value[:, at : at + width] for at in range(0, value.shape[1], width)]
        pieces = [piece.reshape(count, 1, depth, width) for piece in pieces]
        return jnp.concatenate(pieces, axis=1)

    def layer_parts(n):
        return [
            attn_qkv[n].astype(half),
            attn_out[n].astype(half),
            mlp_in[n].astype(half),
            flat(mlp_out[n]),
        ]

    ends = [3 * width, 4 * width, 4 * width + mlp_in.shape[2]]
    ends.append(ends[2] + mlp_out.shape[1] // depth * width)

    def layer_weights(joined):
        return (
            joined[:, : ends[0]],
            joined[:, ends[0] : ends[1]],
            joined[:, ends[1] : ends[2]],
            tall(joined[:, ends[2] : ends[3]]).reshape(-1, width),
        )

    patch_all = gather_rows(jnp.concatenate(layer_parts(0), axis=1))
    byte_all = gather_rows(
        jnp.concatenate(layer_parts(1) + [flat(tables.reshape(-1, width))], axis=1)
    )
    weights = [layer_weights(patch_all), layer_weights(byte_all)]
    qkv_w, out_w, in_w, down_w = ([weights[n][at] for n in range(2)] for at in range(4))
    table_rows = byte_all[:, ends[3] :].reshape(count, tables.shape[0], -1, width)
    table_w = [table_rows[:, n].reshape(-1, width) for n in range(3)]

    mine = patch_proj.shape[0]
    splits = width // mine
    slot, column = rank // splits, rank % splits
    narrow = tables[0].astype(half).reshape(-1, splits, mine).transpose(1, 0, 2)
    narrow = lax.all_to_all(
        jnp.tile(narrow, (count // splits, 1, 1)), ("items", "seq"), 0, 0, tiled=True
    ).reshape(-1, mine)
    all_grid = told[:, 0].reshape(byte_tokens.shape[0] * lax.axis_size("items"), -1, PATCH)
    ahead = jnp.concatenate([jnp.zeros_like(all_grid[:, :1]), all_grid[:, :-1]], axis=1)
    slot_hot = one_hot(pick(ahead, slot, 2), VOCAB, half)
    embed_part = to_half(jnp.dot(slot_hot, narrow, preferred_element_type=single))
    proj_half = patch_proj.astype(half)
    projected_part = jnp.dot(embed_part, proj_half, preferred_element_type=single)
    projected = reduce_group([to_half(projected_part)], width)[0]
    span_rows = byte_tokens.shape[1] // PATCH
    total_patches = doc_ids.shape[1]
    offset = lax.axis_index("seq") * span_rows
    my_pos = offset + jnp.arange(span_rows)
    keep_first = (jnp.arange(PATCH) > 0).astype(single)

    def item_pass(my_bytes, my_groups, all_docs):
        group_hot = one_hot(my_groups, GROUPS, single)
        my_docs = lax.dynamic_slice_in_dim(all_docs, offset, span_rows)
        prior_docs = jnp.concatenate(
            [lax.dynamic_slice_in_dim(all_docs, jnp.maximum(offset - 1, 0), 1), my_docs[:-1]]
        )
        starts = (my_pos == 0) | (my_docs != prior_docs)

        allowed = (jnp.arange(total_patches)[None, :] <= my_pos[:, None]) & (
            all_docs[None, :] == my_docs[:, None]
        )
        bias = jnp.where(allowed, 0.0, NEGATIVE)
        narrow_spec = pl.BlockSpec((span_rows, LANES), lambda at: (0, at))

        def global_forward(qkv_half):
            both_all = gather_seq(qkv_half[:, width:])
            mixed = by_heads(
                patch_forward_kernel,
                jax.ShapeDtypeStruct((span_rows, width), half),
                narrow_spec,
                qkv_half,
                both_all,
                bias,
            )
            return (mixed, both_all)

        def global_backward(grad_half, qkv_half, both_all, mixed):
            seq = lax.axis_size("seq")
            query_grad, both_grad = by_heads(
                patch_backward_kernel,
                (
                    jax.ShapeDtypeStruct((span_rows, width), half),
                    jax.ShapeDtypeStruct((seq, 2, span_rows, width), half),
                ),
                (
                    narrow_spec,
                    pl.BlockSpec((seq, 2, span_rows, LANES), lambda at: (0, 0, 0, at)),
                ),
                qkv_half,
                both_all,
                bias,
                grad_half,
            )
            pairs = both_grad.reshape(seq // 2, 2, 2, span_rows, width)
            core = lax.axis_index("seq") % 2
            got = swap(pick(pairs, 1 - core, 1), "seq", 1)
            key_value_grad = to_half(along_depth(wide(pick(pairs, core, 1)) + wide(got)))
            return jnp.concatenate([query_grad, key_value_grad[0], key_value_grad[1]], axis=1)

        byte_grid = my_bytes.reshape(span_rows, PATCH)
        resid = jnp.where(starts[:, None], vectors[5][None, :], projected)
        top, saved_top = layer_forward(
            resid, vectors[0:2], qkv_w[0], out_w[0], in_w[0], down_w[0], global_forward
        )
        patch_sides = gather_rows(
            jnp.concatenate([saved_top[2], saved_top[5], saved_top[9]], axis=1)
        )
        top, active_columns = lax.optimization_barrier((top, deal_columns([saved_top[11]])[0]))
        before = jnp.concatenate([jnp.zeros((span_rows, 1), jnp.int32), byte_grid[:, :-1]], axis=1)
        before_hot = one_hot(before, VOCAB, half)
        local_embed = jnp.dot(before_hot, table_w[1], preferred_element_type=single).reshape(
            span_rows, PATCH, width
        )
        local_in = (
            local_embed * keep_first[None, :, None] + top[:, None, :] + vectors[6 : 6 + PATCH][None]
        )
        result, saved_low = layer_forward(
            local_in.reshape(span_rows * PATCH, width),
            vectors[2:4],
            qkv_w[1],
            out_w[1],
            in_w[1],
            down_w[1],
            local_forward,
        )
        final, (final_normed, final_scale) = norm_forward(result, vectors[4])
        final_half = final.astype(half)
        logits = jnp.einsum("rd,vd->rv", final_half, table_w[2], preferred_element_type=single)
        shifted = logits - jnp.max(logits, axis=-1, keepdims=True)
        totals = jnp.sum(jnp.exp(shifted), axis=-1, keepdims=True)
        probs = jnp.exp(shifted) / totals
        target_hot = one_hot(my_bytes, VOCAB, single)
        losses = jnp.log(totals[:, 0]) - jnp.sum(shifted * target_hot, axis=-1)
        loss_terms = jnp.sum(losses[:, None] * group_hot, axis=0)
        row_weight = jnp.sum(group_hot * (1.0 / (GROUPS * counts))[None, :], axis=-1)
        logit_half = (row_weight[:, None] * (probs - target_hot)).astype(half)
        head_grad = jnp.einsum("rv,rd->vd", logit_half, final_half, preferred_element_type=single)
        final_grad = jnp.einsum("rv,vd->rd", logit_half, table_w[2], preferred_element_type=single)
        result_grad, final_gain_grad = norm_backward(
            final_grad, final_normed, final_scale, vectors[4]
        )
        running, sides = {}, {}

        def after_low(where, value, *others):
            if where == "mlp":
                grads = [to_half(outer(pair)) for pair in others]
                running["early"] = Stepped(group_steps(grads + [to_half(head_grad)], width))
            elif where == "projections":
                attn_half, mixed_half, proj_half = others
                value, sides["all"] = lax.optimization_barrier((value, patch_sides))
                value, proj_half = advance([value, proj_half], running["early"])
                sides["qkv"], sides["out"] = (attn_half, value), (mixed_half, proj_half)
                return value
            (value,) = advance([value], running["early"])
            return value

        def after_top(where, value, *others):
            if where == "mlp":
                sides["mlp"] = others[0][1]
                (value,) = advance([value], running["low"])
            elif where == "attention":
                (value,) = advance([value], running["early"], running["low"])
            elif where == "projections":
                value, sides["top"] = lax.optimization_barrier((value, top_all))
                (value,) = tie([value], [running["low"]])
                sides["patch"] = [value, others[2], sides["mlp"]]
            return value

        local_grad, low_gains = layer_backward(
            result_grad,
            saved_low,
            vectors[2:4],
            qkv_w[1],
            out_w[1],
            in_w[1],
            down_w[1],
            local_backward,
            after_low,
        )
        grid_grad = local_grad.reshape(span_rows, PATCH, width)
        top_grad = jnp.sum(grid_grad, axis=1)
        position_grad = jnp.sum(grid_grad, axis=0)
        masked_grad = (grid_grad * keep_first[None, :, None]).reshape(span_rows * PATCH, width)
        local_table_grad = hot_sum(before_hot, masked_grad)
        top_all = gather_rows(to_half(top_grad))
        low_partials = [to_half(outer(sides["qkv"])), to_half(outer(sides["out"]))]
        running["low"] = Stepped(
            group_steps(low_partials + [to_half(local_table_grad)], width, deal=False)
        )
        (top_grad,) = advance([top_grad], running["low"])
        resid_grad, top_gains = layer_backward(
            top_grad,
            saved_top,
            vectors[0:2],
            qkv_w[0],
            out_w[0],
            in_w[0],
            down_w[0],
            global_backward,
            after_top,
        )
        start_grad = jnp.sum(jnp.where(starts[:, None], resid_grad, 0.0), axis=0)
        projected_half = jnp.where(starts[:, None], 0.0, resid_grad).astype(half)
        vector_grad = jnp.concatenate(
            [top_gains, low_gains, final_gain_grad[None], start_grad[None], position_grad],
            axis=0,
        )
        own = jnp.broadcast_to(
            projected_half[None], (lax.axis_size("seq") // 2,) + projected_half.shape
        )
        joint = deal_depth(jnp.concatenate([own, running["low"].held[0]], axis=1))
        joint, *patch = lax.optimization_barrier((joint, *sides["patch"]))
        running["low"].feed([joint[:, span_rows:]])
        running["gather"] = Stepped(gather_steps(joint[:, :span_rows]))
        advance([], running["gather"])
        columns = deal_columns(patch)
        patch_down = outer((active_columns, sides["top"]))
        (patch_down,) = advance([patch_down], running["gather"])
        columns = advance(columns, running["gather"])
        attn_all, mixed_all, mlp_all = (
            sides["all"][:, at * width : (at + 1) * width] for at in range(3)
        )
        blocks = [outer(pair) for pair in zip((attn_all, mixed_all, mlp_all), columns)]
        blocks = advance([to_half(part) for part in blocks], running["gather"])
        patch_qkv, patch_out, patch_in = deal_rows(blocks)
        projected_all = running["gather"].result
        proj_grad = jnp.einsum(
            "ri,rd->id", embed_part, projected_all, preferred_element_type=single
        )
        embed_grad = jnp.einsum(
            "rd,id->ri", projected_all, proj_half, preferred_element_type=single
        )
        slot_grad = hot_sum(slot_hot, embed_grad)
        slot_grad, patch_qkv, patch_out, patch_in = lax.optimization_barrier(
            (slot_grad, patch_qkv, patch_out, patch_in)
        )
        slot_size, vector_rows = slot_grad.size // count, spread(vector_grad.reshape(-1))
        dealt = lax.all_to_all(
            jnp.concatenate([slot_grad.reshape(count, slot_size), vector_rows], axis=1),
            ("items", "seq"),
            0,
            0,
            tiled=True,
        )
        vector_piece = jnp.sum(dealt[:, slot_size:], axis=0)
        slot_rows = dealt[:, :slot_size].reshape(count, -1, mine)
        slot_rows = jnp.sum(slot_rows.reshape(PATCH, splits, -1, mine), axis=0)
        global_table_grad = slot_rows.transpose(1, 0, 2).reshape(-1, width)
        assert all(group.result is not None for group in running.values())
        early, low = running["early"].result, running["low"].result
        owned = (
            proj_grad,
            jnp.stack([global_table_grad, low[2], early[2]]),
            jnp.stack([patch_qkv, low[0]]),
            jnp.stack([patch_out, low[1]]),
            jnp.stack([patch_in, early[0]]),
            jnp.stack([patch_down, early[1]]),
        )
        return (loss_terms, owned, vector_piece)

    loss_terms, owned, vector_piece = item_pass(byte_tokens[0], groups[0], doc_ids[0])
    shard_square = sum((jnp.sum(piece * piece) for piece in owned))
    shard_square = shard_square + jnp.sum(vector_piece * vector_piece)
    tail = share(jnp.concatenate([vector_piece, shard_square[None], loss_terms]))
    size = vector_piece.shape[0]
    vector_total = tail[:, :size].reshape(-1)[: vectors.size].reshape(vectors.shape)
    loss_total = jnp.sum(tail[:, size + 1 :], axis=0)
    loss = jnp.sum(loss_total / counts) / GROUPS
    grad_norm = jnp.sqrt(jnp.sum(tail[:, size]))
    factor = jnp.minimum(1.0, CLIP_AT / grad_norm)
    step = float(STEP_NUMBER)
    rates = (
        (PATCH * D) ** (-0.5),
        jnp.array([1.0, 1.0, 2.0 * D ** (-0.5)], single).reshape(3, 1, 1),
        D ** (-0.5),
        (D // 8) ** (-0.5),
        D ** (-0.5),
        FF ** (-0.5),
        0.5,
    )
    masters = (patch_proj, tables, attn_qkv, attn_out, mlp_in, mlp_out, vectors)
    grads = tuple(owned) + (vector_total,)
    firsts = (first_proj, first_tables, first_qkv, first_out, first_in, first_down, first_vectors)
    seconds = (
        second_proj,
        second_tables,
        second_qkv,
        second_out,
        second_in,
        second_down,
        second_vectors,
    )
    done = [
        adam_step(masters[n], grads[n] * factor, firsts[n], seconds[n], rates[n], step)
        for n in range(7)
    ]
    return (
        loss,
        grad_norm,
        done[0][0],
        done[1][0],
        done[2][0],
        done[3][0],
        done[4][0],
        done[5][0],
        done[6][0],
        done[0][1],
        done[1][1],
        done[2][1],
        done[3][1],
        done[4][1],
        done[5][1],
        done[6][1],
        done[0][2],
        done[1][2],
        done[2][2],
        done[3][2],
        done[4][2],
        done[5][2],
        done[6][2],
    )


def solution(mesh):
    return jax.shard_map(
        body,
        mesh=mesh,
        in_specs=(
            P("items", "seq"),
            P("items", "seq"),
            P("items", None),
            P(("items", "seq"), None),
            P(None, ("items", "seq"), None),
            P(None, ("items", "seq"), None),
            P(None, ("items", "seq"), None),
            P(None, ("items", "seq"), None),
            P(None, ("items", "seq"), None),
            P(),
            P(("items", "seq"), None),
            P(None, ("items", "seq"), None),
            P(None, ("items", "seq"), None),
            P(None, ("items", "seq"), None),
            P(None, ("items", "seq"), None),
            P(None, ("items", "seq"), None),
            P(),
            P(("items", "seq"), None),
            P(None, ("items", "seq"), None),
            P(None, ("items", "seq"), None),
            P(None, ("items", "seq"), None),
            P(None, ("items", "seq"), None),
            P(None, ("items", "seq"), None),
            P(),
        ),
        out_specs=(
            P(),
            P(),
            P(("items", "seq"), None),
            P(None, ("items", "seq"), None),
            P(None, ("items", "seq"), None),
            P(None, ("items", "seq"), None),
            P(None, ("items", "seq"), None),
            P(None, ("items", "seq"), None),
            P(),
            P(("items", "seq"), None),
            P(None, ("items", "seq"), None),
            P(None, ("items", "seq"), None),
            P(None, ("items", "seq"), None),
            P(None, ("items", "seq"), None),
            P(None, ("items", "seq"), None),
            P(),
            P(("items", "seq"), None),
            P(None, ("items", "seq"), None),
            P(None, ("items", "seq"), None),
            P(None, ("items", "seq"), None),
            P(None, ("items", "seq"), None),
            P(None, ("items", "seq"), None),
            P(),
        ),
        check_vma=False,
    )
```

```python
import jax
import jax.numpy as jnp
from jax import lax
from jax.experimental import pallas as pl
from jax.experimental.pallas import tpu as pltpu
from jax.sharding import PartitionSpec as P

D = 768
HEAD_DIM = 64
FF = 3072
PATCH = 8
VOCAB = 256
GROUPS = 4
STEP_NUMBER = 7


EPSILON = 1e-05
CLIP_AT = 0.01
BETA_ONE = 0.9
BETA_TWO = 0.95
ADAM_EPS = 1e-08
DECAY = 0.1
NEGATIVE = -1e30


def norm_forward(values, gain):
    scale = lax.rsqrt(jnp.mean(values * values, axis=-1, keepdims=True) + EPSILON)
    normed = values * scale
    return (normed * gain, (normed, scale))


def norm_backward(upstream, normed, scale, gain):
    gain_grad = jnp.sum(upstream * normed, axis=0)
    inner = upstream * gain
    return (scale * (inner - normed * jnp.mean(inner * normed, axis=-1, keepdims=True)), gain_grad)


def to_half(value):
    return value.astype(jnp.bfloat16)


def wide(value):
    return value.astype(jnp.float32)


def pick(value, index, axis):
    return lax.dynamic_index_in_dim(value, index, axis, keepdims=False)


def swap(value, axis, bit):
    count = lax.axis_size(axis)
    return lax.ppermute(value, axis, [(at, at ^ bit) for at in range(count)])


def same_core():
    seq = lax.axis_size("seq")
    return [list(range(first, seq, 2)) for first in range(2)]


def deal_depth(value):
    return lax.all_to_all(
        to_half(value), "seq", 0, 0, axis_index_groups=same_core(), tiled=True
    )


def along_depth(value):
    return jnp.sum(wide(deal_depth(value)), axis=0)


def gather_seq(value):
    seq = lax.axis_size("seq")
    mine = lax.all_to_all(
        jnp.broadcast_to(value[None], (seq // 2,) + value.shape),
        "seq",
        0,
        0,
        axis_index_groups=same_core(),
        tiled=True,
    )
    other = swap(mine, "seq", 1)
    second = lax.axis_index("seq") % 2 == 1
    pair = jnp.stack([jnp.where(second, other, mine), jnp.where(second, mine, other)], axis=1)
    return pair.reshape(seq * value.shape[0], value.shape[1])


def group_steps(partials, width, deal=True):
    items, seq = lax.axis_size("items"), lax.axis_size("seq")
    at_item, at_seq = lax.axis_index("items"), lax.axis_index("seq")
    core, x_at, y_at = at_seq % 2, at_item % 2, at_item // 2
    depth = seq // 2
    grids = [
        part.reshape(items // 2, 2, depth, 2, part.shape[0] // (items * seq), part.shape[1])
        for part in partials
    ]

    def side(index):
        return jnp.concatenate(
            [
                pick(grid, index, 3)[..., begin : begin + width]
                for grid in grids
                for begin in range(0, grid.shape[-1], width)
            ],
            axis=3,
        )

    kept = side(core)
    (sent,) = yield (side(1 - core),)
    (got,) = yield (swap(sent, "seq", 1),)
    rows = kept.shape[3]
    cut = rows // 16 * 8
    halves = ((0, cut), (cut, rows))

    def cells(value, y_from, y_count, x_from, x_count, half):
        begin, end = halves[half]
        return lax.dynamic_slice(
            value,
            (y_from, x_from, 0, begin, 0),
            (y_count, x_count, depth, end - begin, width),
        )

    def pair_sum(*where):
        return wide(cells(kept, *where)) + wide(cells(got, *where))

    to_x, to_y = yield (
        to_half(pair_sum(0, 2, 1 - x_at, 1, 0)),
        to_half(pair_sum(1 - y_at, 1, 0, 2, 1)),
    )
    first_in, second_in = yield swap(to_x, "items", 1), swap(to_y, "items", 2)
    to_y, to_x = yield (
        to_half(
            pair_sum(1 - y_at, 1, x_at, 1, 0)
            + wide(lax.dynamic_slice_in_dim(first_in, 1 - y_at, 1, 0))
        ),
        to_half(
            pair_sum(y_at, 1, 1 - x_at, 1, 1)
            + wide(lax.dynamic_slice_in_dim(second_in, 1 - x_at, 1, 1))
        ),
    )
    first_end, second_end = yield swap(to_y, "items", 2), swap(to_x, "items", 1)
    first = (
        pair_sum(y_at, 1, x_at, 1, 0)
        + wide(lax.dynamic_slice_in_dim(first_in, y_at, 1, 0))
        + wide(first_end)
    )
    second = (
        pair_sum(y_at, 1, x_at, 1, 1)
        + wide(lax.dynamic_slice_in_dim(second_in, x_at, 1, 1))
        + wide(second_end)
    )
    (blocks,) = yield (
        jnp.concatenate([to_half(first[0, 0]), to_half(second[0, 0])], axis=1),
    )
    if deal:
        (blocks,) = yield (deal_depth(blocks),)
    rows = jnp.sum(wide(blocks), axis=0)
    out, at = [], 0
    for grid in grids:
        deep, pieces = grid.shape[4], []
        for _ in range(0, grid.shape[-1], width):
            pieces.append(rows[at : at + deep])
            at += deep
        out.append(jnp.concatenate(pieces, axis=1))
    return out


def in_order(mine, other, bit, axis):
    return jnp.stack(
        [jnp.where(bit == 1, other, mine), jnp.where(bit == 1, mine, other)], axis=axis
    )


def gather_steps(mine):
    items, seq = lax.axis_size("items"), lax.axis_size("seq")
    at_item, at_seq = lax.axis_index("items"), lax.axis_index("seq")
    core, x_at, y_at = at_seq % 2, at_item % 2, at_item // 2
    rows, width = mine.shape[1:]
    cut = width // 2
    first, second = yield (mine[..., :cut], mine[..., cut:])
    to_x, to_y = yield (swap(first, "items", 1), swap(second, "items", 2))
    first, second = yield (in_order(first, to_x, x_at, 0), in_order(second, to_y, y_at, 0))
    to_y, to_x = yield (swap(first, "items", 2), swap(second, "items", 1))
    (mine,) = yield (
        jnp.concatenate(
            [in_order(first, to_y, y_at, 0), in_order(second, to_x, x_at, 1)], axis=-1
        ),
    )
    (other,) = yield (swap(mine, "seq", 1),)
    return in_order(mine, other, core, 3).reshape(items * seq * rows, width)


class Stepped:
    def __init__(self, steps):
        self.steps = steps
        self.held = next(self.steps)
        self.sending = True
        self.result = None

    def feed(self, arrays):
        try:
            self.held = self.steps.send(tuple(arrays))
        except StopIteration as end:
            self.held, self.result = (), end.value
        self.sending = not self.sending


def tie(values, groups):
    flat = list(values)
    for group in groups:
        flat.extend(group.held)
    flat = list(lax.optimization_barrier(tuple(flat)))
    values, flat = flat[: len(values)], flat[len(values) :]
    for group in groups:
        size = len(group.held)
        group.feed(flat[:size])
        flat = flat[size:]
    return values


def advance(values, *groups):
    waiting = [group for group in groups if group.result is None and not group.sending]
    if waiting:
        values = tie(values, waiting)
    sending = [group for group in groups if group.result is None]
    return tie(values, sending) if sending else values


def reduce_group(partials, width):
    group = Stepped(group_steps(partials, width))
    while group.result is None:
        advance([], group)
    return group.result


def to_depth(value):
    half_seq = lax.axis_size("seq") // 2
    return deal_depth(jnp.broadcast_to(value[None], (half_seq,) + value.shape))


def gather_swaps(mine):
    group = Stepped(gather_steps(mine))
    while group.result is None:
        advance([], group)
    return group.result


def share(row):
    count = lax.axis_size("items") * lax.axis_size("seq")
    return lax.all_to_all(
        jnp.broadcast_to(row[None], (count,) + row.shape), ("items", "seq"), 0, 0, tiled=True
    )


def spread(value):
    count = lax.axis_size("items") * lax.axis_size("seq")
    size = -(-value.shape[0] // count)
    return jnp.pad(value, (0, size * count - value.shape[0])).reshape(count, size)


def gather_rows(value):
    return lax.all_gather(value, ("items", "seq"), axis=0, tiled=True)


def one_hot(indices, width, dtype):
    return (indices.reshape(-1)[:, None] == jnp.arange(width)[None, :]).astype(dtype)


def hot_sum(hot, value):
    high = to_half(value)
    rest = to_half(value - wide(high))
    add = lambda term: jnp.einsum("rv,rd->vd", hot, term, preferred_element_type=jnp.float32)
    return add(high) + add(rest)


def layer_forward(resid, gains, qkv_w, out_w, in_w, down_w, attend):
    attn_in, (normed_one, scale_one) = norm_forward(resid, gains[0])
    attn_half = attn_in.astype(jnp.bfloat16)
    qkv_half = jnp.dot(attn_half, qkv_w, preferred_element_type=jnp.float32).astype(jnp.bfloat16)
    mixed, kept = attend(qkv_half)
    mixed_half = mixed.astype(jnp.bfloat16)
    middle = resid + jnp.dot(mixed_half, out_w, preferred_element_type=jnp.float32)
    mlp_norm, (normed_two, scale_two) = norm_forward(middle, gains[1])
    mlp_half = mlp_norm.astype(jnp.bfloat16)
    hidden = jnp.dot(mlp_half, in_w, preferred_element_type=jnp.float32)
    active_half = jax.nn.gelu(hidden).astype(jnp.bfloat16)
    result = middle + jnp.dot(active_half, down_w, preferred_element_type=jnp.float32)
    saved = (
        normed_one,
        scale_one,
        attn_half,
        qkv_half,
        mixed,
        mixed_half,
        kept,
        normed_two,
        scale_two,
        mlp_half,
        hidden,
        active_half,
    )
    return (result, saved)


def layer_backward(result_grad, saved, gains, qkv_w, out_w, in_w, down_w, attend_back, after):
    (
        normed_one,
        scale_one,
        attn_half,
        qkv_half,
        mixed,
        mixed_half,
        kept,
        normed_two,
        scale_two,
        mlp_half,
        hidden,
        active_half,
    ) = saved
    branch_half = result_grad.astype(jnp.bfloat16)
    active_grad = jnp.einsum("rd,fd->rf", branch_half, down_w, preferred_element_type=jnp.float32)
    _, gelu_back = jax.vjp(jax.nn.gelu, hidden)
    hidden_half = gelu_back(active_grad)[0].astype(jnp.bfloat16)
    hidden_half = after("mlp", hidden_half, (mlp_half, hidden_half), (active_half, branch_half))
    mlp_grad = jnp.einsum("rf,df->rd", hidden_half, in_w, preferred_element_type=jnp.float32)
    middle_grad, gain_two = norm_backward(mlp_grad, normed_two, scale_two, gains[1])
    middle_grad = middle_grad + result_grad
    proj_half = middle_grad.astype(jnp.bfloat16)
    mixed_grad = jnp.einsum("rd,ed->re", proj_half, out_w, preferred_element_type=jnp.float32)
    mixed_grad_half = after("attention", mixed_grad.astype(jnp.bfloat16))
    qkv_grad_half = attend_back(mixed_grad_half, qkv_half, kept, mixed).astype(jnp.bfloat16)
    qkv_grad_half = after("projections", qkv_grad_half, attn_half, mixed_half, proj_half)
    attn_grad = jnp.einsum("re,de->rd", qkv_grad_half, qkv_w, preferred_element_type=jnp.float32)
    resid_grad, gain_one = norm_backward(attn_grad, normed_one, scale_one, gains[0])
    resid_grad = after("end", resid_grad + middle_grad)
    return resid_grad, jnp.stack([gain_one, gain_two])


def outer(pair):
    return jnp.einsum("ri,rj->ij", *pair, preferred_element_type=jnp.float32)


def column_blocks(parts):
    count = lax.axis_size("items") * lax.axis_size("seq")
    rows = parts[0].shape[0]
    blocks = jnp.concatenate([part.reshape(rows, count, -1) for part in parts], axis=2)
    return blocks.transpose(1, 0, 2)


def deal_columns(blocks, parts):
    count, rows = blocks.shape[:2]
    dealt = lax.all_to_all(blocks, ("items", "seq"), 0, 0, tiled=True).reshape(count * rows, -1)
    out, at = [], 0
    for part in parts:
        size = part.shape[1] // count
        out.append(dealt[:, at : at + size])
        at += size
    return out


def deal_rows(parts):
    count = lax.axis_size("items") * lax.axis_size("seq")
    blocks = jnp.concatenate([to_half(part) for part in parts], axis=1)
    return lax.all_to_all(
        blocks.reshape(count, -1, blocks.shape[1]), ("items", "seq"), 0, 0, tiled=True
    )


def whole_rows(dealt, parts):
    out, at = [], 0
    for part in parts:
        size = part.shape[1]
        piece = dealt[:, :, at : at + size].transpose(1, 0, 2)
        out.append(wide(piece.reshape(piece.shape[0], -1)))
        at += size
    return out


ROWS = 128
LANES = 128


def contract(left, right, left_dim, right_dim):
    return lax.dot_general(
        left, right, (((left_dim,), (right_dim,)), ((), ())), preferred_element_type=jnp.float32
    )


def local_masks():
    row = lax.broadcasted_iota(jnp.int32, (ROWS, ROWS), 0)
    column = lax.broadcasted_iota(jnp.int32, (ROWS, ROWS), 1)
    allowed = (row // PATCH == column // PATCH) & (column <= row)
    lane = lax.broadcasted_iota(jnp.int32, (ROWS, LANES), 1)
    lanes = [
        jnp.where(lane // HEAD_DIM == head, 1.0, 0.0).astype(jnp.bfloat16)
        for head in range(LANES // HEAD_DIM)
    ]
    return allowed, lanes


def local_probs(query, key, allowed):
    scores = contract(query, key, 1, 1) * HEAD_DIM ** (-0.5)
    scores = jnp.where(allowed, scores, NEGATIVE)
    raised = jnp.exp(scores - jnp.max(scores, axis=-1, keepdims=True))
    return raised / jnp.sum(raised, axis=-1, keepdims=True)


def local_forward_kernel(qkv_ref, mixed_ref):
    width = mixed_ref.shape[1]
    allowed, lanes = local_masks()
    for begin in range(0, width, LANES):
        query, key, value = (
            qkv_ref[:, part * width + begin : part * width + begin + LANES] for part in range(3)
        )
        mixed = jnp.zeros((ROWS, LANES), jnp.float32)
        for mask in lanes:
            probs = local_probs(query * mask, key, allowed).astype(jnp.bfloat16)
            mixed = mixed + contract(probs, value * mask, 1, 0)
        mixed_ref[:, begin : begin + LANES] = mixed.astype(jnp.bfloat16)


def local_backward_kernel(qkv_ref, grad_ref, out_ref):
    width = grad_ref.shape[1]
    allowed, lanes = local_masks()
    scale = HEAD_DIM ** (-0.5)
    for begin in range(0, width, LANES):
        query, key, value = (
            qkv_ref[:, part * width + begin : part * width + begin + LANES] for part in range(3)
        )
        upstream = grad_ref[:, begin : begin + LANES]
        sums = [jnp.zeros((ROWS, LANES), jnp.float32) for _ in range(3)]
        for mask in lanes:
            head_query, head_upstream = query * mask, upstream * mask
            probs = local_probs(head_query, key, allowed)
            prob_grad = contract(head_upstream, value, 1, 1)
            inner = jnp.sum(prob_grad * probs, axis=-1, keepdims=True)
            score_half = (probs * (prob_grad - inner)).astype(jnp.bfloat16)
            sums[0] = sums[0] + contract(score_half, key * mask, 1, 0)
            sums[1] = sums[1] + contract(score_half, head_query, 0, 0)
            sums[2] = sums[2] + contract(probs.astype(jnp.bfloat16), head_upstream, 0, 0)
        for part, factor in enumerate((scale, scale, 1.0)):
            at = part * width + begin
            out_ref[:, at : at + LANES] = (sums[part] * factor).astype(jnp.bfloat16)


def by_rows(kernel, out_width, *operands):
    rows = operands[0].shape[0]
    moved = sum(value.size for value in operands) * 2 + rows * out_width * 2
    return pl.pallas_call(
        kernel,
        grid=(rows // ROWS,),
        in_specs=[pl.BlockSpec((ROWS, value.shape[1]), lambda at: (at, 0)) for value in operands],
        out_specs=pl.BlockSpec((ROWS, out_width), lambda at: (at, 0)),
        out_shape=jax.ShapeDtypeStruct((rows, out_width), jnp.bfloat16),
        cost_estimate=pl.CostEstimate(
            flops=rows * ROWS * out_width * 8, bytes_accessed=moved, transcendentals=rows * ROWS
        ),
    )(*operands)


def local_forward(qkv_half):
    return by_rows(local_forward_kernel, qkv_half.shape[1] // 3, qkv_half), None


def local_backward(grad_half, qkv_half, kept, mixed):
    return by_rows(local_backward_kernel, qkv_half.shape[1], qkv_half, grad_half)


def patch_probs(query, key, bias):
    scores = contract(query, key, 1, 1) * HEAD_DIM ** (-0.5) + bias
    raised = jnp.exp(scores - jnp.max(scores, axis=-1, keepdims=True))
    return raised / jnp.sum(raised, axis=-1, keepdims=True)


def head_lanes():
    lane = lax.broadcasted_iota(jnp.int32, (1, LANES), 1)
    return [
        jnp.where(lane // HEAD_DIM == head, 1.0, 0.0).astype(jnp.bfloat16)
        for head in range(LANES // HEAD_DIM)
    ]


def patch_forward_kernel(query_ref, key_ref, value_ref, bias_ref, mixed_ref):
    mixed = jnp.zeros(mixed_ref.shape, jnp.float32)
    for mask in head_lanes():
        probs = patch_probs(query_ref[...] * mask, key_ref[...], bias_ref[...])
        mixed = mixed + contract(probs.astype(jnp.bfloat16), value_ref[...] * mask, 1, 0)
    mixed_ref[...] = mixed.astype(jnp.bfloat16)


def patch_backward_kernel(query_ref, key_ref, value_ref, bias_ref, grad_ref, query_out, both_out):
    seq, _, span, _ = both_out.shape
    query_grad = jnp.zeros(query_out.shape, jnp.float32)
    key_grad = jnp.zeros(key_ref.shape, jnp.float32)
    value_grad = jnp.zeros(key_ref.shape, jnp.float32)
    for mask in head_lanes():
        query, upstream, key = query_ref[...] * mask, grad_ref[...] * mask, key_ref[...]
        probs = patch_probs(query, key, bias_ref[...])
        prob_grad = contract(upstream, value_ref[...], 1, 1)
        inner = jnp.sum(prob_grad * probs, axis=-1, keepdims=True)
        score_half = (probs * (prob_grad - inner)).astype(jnp.bfloat16)
        query_grad = query_grad + contract(score_half, key * mask, 1, 0)
        key_grad = key_grad + contract(score_half, query, 0, 0)
        value_grad = value_grad + contract(probs.astype(jnp.bfloat16), upstream, 0, 0)
    scale = HEAD_DIM ** (-0.5)
    query_out[...] = (query_grad * scale).astype(jnp.bfloat16)
    both_out[:, 0] = (key_grad * scale).astype(jnp.bfloat16).reshape(seq, span, LANES)
    both_out[:, 1] = value_grad.astype(jnp.bfloat16).reshape(seq, span, LANES)


def by_heads(kernel, out_shape, out_specs, qkv_half, both_all, bias, *others):
    rows, total, pairs = qkv_half.shape[0], both_all.shape[0], both_all.shape[1] // 2 // LANES
    columns = lambda count, shift: pl.BlockSpec((count, LANES), lambda at: (0, at + shift))
    return pl.pallas_call(
        kernel,
        grid=(pairs,),
        in_specs=[
            columns(rows, 0),
            columns(total, 0),
            columns(total, pairs),
            pl.BlockSpec((rows, total), lambda at: (0, 0)),
        ]
        + [columns(rows, 0) for _ in others],
        out_specs=out_specs,
        out_shape=out_shape,
    )(qkv_half, both_all, both_all, bias, *others)


def adam_step(weight, grad, first, second, rate, count):
    first = BETA_ONE * first + (1.0 - BETA_ONE) * grad
    second = BETA_TWO * second + (1.0 - BETA_TWO) * grad * grad
    first_hat = first / (1.0 - BETA_ONE**count)
    second_hat = second / (1.0 - BETA_TWO**count)
    return (
        weight - rate * (first_hat / (jnp.sqrt(second_hat) + ADAM_EPS) + DECAY * weight),
        first,
        second,
    )


def body(
    byte_tokens,
    groups,
    doc_ids,
    patch_proj,
    tables,
    attn_qkv,
    attn_out,
    mlp_in,
    mlp_out,
    vectors,
    first_proj,
    first_tables,
    first_qkv,
    first_out,
    first_in,
    first_down,
    first_vectors,
    second_proj,
    second_tables,
    second_qkv,
    second_out,
    second_in,
    second_down,
    second_vectors,
):
    half = jnp.bfloat16
    single = jnp.float32
    width = vectors.shape[1]
    depth = attn_qkv.shape[1]
    count = lax.axis_size("items") * lax.axis_size("seq")
    rank = lax.axis_index("items") * lax.axis_size("seq") + lax.axis_index("seq")
    mine = patch_proj.shape[0]
    splits = width // mine
    slot, column = rank // splits, rank % splits
    narrow = tables[0].astype(half).reshape(-1, splits, mine).transpose(1, 0, 2)
    narrow = jnp.tile(narrow.reshape(splits, -1), (count // splits, 1))
    own = jnp.concatenate([byte_tokens.reshape(-1), groups.reshape(-1)]).astype(half)
    patch_mine = to_depth(jnp.concatenate([attn_qkv[0], attn_out[0]], axis=1).astype(half))
    patch_mine, own = lax.optimization_barrier((patch_mine, own))
    dealt = lax.all_to_all(
        jnp.concatenate([narrow, jnp.broadcast_to(own[None], (count,) + own.shape)], axis=1),
        ("items", "seq"),
        0,
        0,
        tiled=True,
    )
    told = dealt[:, narrow.shape[1] :].astype(jnp.int32).reshape(count, 2, -1)
    narrow = dealt[:, : narrow.shape[1]].reshape(-1, mine)
    counts = jnp.sum(one_hot(told[:, 1], GROUPS, single), axis=0)

    def flat(value):
        return jnp.concatenate(
            [value[at : at + depth] for at in range(0, value.shape[0], depth)], axis=1
        ).astype(half)

    def tall(value):
        pieces = [value[:, at : at + width] for at in range(0, value.shape[1], width)]
        pieces = [piece.reshape(count, 1, depth, width) for piece in pieces]
        return jnp.concatenate(pieces, axis=1)

    def layer_parts(n):
        return [
            attn_qkv[n].astype(half),
            attn_out[n].astype(half),
            mlp_in[n].astype(half),
            flat(mlp_out[n]),
        ]

    sizes = [3 * width, width, mlp_in.shape[2], mlp_out.shape[1] // depth * width]

    def cut(joined, begin, lengths):
        pieces = []
        for length in lengths:
            pieces.append(joined[:, begin : begin + length])
            begin += length
        return pieces

    patch_parts, byte_parts = layer_parts(0), layer_parts(1)
    patch_all = gather_swaps(patch_mine)
    rest_all = gather_rows(
        jnp.concatenate(
            patch_parts[2:] + byte_parts + [flat(tables.reshape(-1, width))], axis=1
        )
    )
    rest = cut(rest_all, 0, sizes[2:] + sizes + [tables.shape[0] * tables.shape[1] // depth * width])
    weights = [cut(patch_all, 0, sizes[:2]) + rest[:2], rest[2:6]]
    for part in weights:
        part[3] = tall(part[3]).reshape(-1, width)
    qkv_w, out_w, in_w, down_w = ([weights[n][at] for n in range(2)] for at in range(4))
    table_rows = rest[6].reshape(count, tables.shape[0], -1, width)
    table_w = [table_rows[:, n].reshape(-1, width) for n in range(3)]

    all_grid = told[:, 0].reshape(byte_tokens.shape[0] * lax.axis_size("items"), -1, PATCH)
    ahead = jnp.concatenate([jnp.zeros_like(all_grid[:, :1]), all_grid[:, :-1]], axis=1)
    slot_hot = one_hot(pick(ahead, slot, 2), VOCAB, half)
    embed_part = to_half(jnp.dot(slot_hot, narrow, preferred_element_type=single))
    proj_half = patch_proj.astype(half)
    projected_part = jnp.dot(embed_part, proj_half, preferred_element_type=single)
    projected = reduce_group([to_half(projected_part)], width)[0]
    span_rows = byte_tokens.shape[1] // PATCH
    total_patches = doc_ids.shape[1]
    offset = lax.axis_index("seq") * span_rows
    my_pos = offset + jnp.arange(span_rows)
    keep_first = (jnp.arange(PATCH) > 0).astype(single)

    def item_pass(my_bytes, my_groups, all_docs):
        group_hot = one_hot(my_groups, GROUPS, single)
        my_docs = lax.dynamic_slice_in_dim(all_docs, offset, span_rows)
        prior_docs = jnp.concatenate(
            [lax.dynamic_slice_in_dim(all_docs, jnp.maximum(offset - 1, 0), 1), my_docs[:-1]]
        )
        starts = (my_pos == 0) | (my_docs != prior_docs)

        allowed = (jnp.arange(total_patches)[None, :] <= my_pos[:, None]) & (
            all_docs[None, :] == my_docs[:, None]
        )
        bias = jnp.where(allowed, 0.0, NEGATIVE)
        narrow_spec = pl.BlockSpec((span_rows, LANES), lambda at: (0, at))

        def global_forward(qkv_half):
            both_all = gather_seq(qkv_half[:, width:])
            mixed = by_heads(
                patch_forward_kernel,
                jax.ShapeDtypeStruct((span_rows, width), half),
                narrow_spec,
                qkv_half,
                both_all,
                bias,
            )
            return (mixed, both_all)

        def global_backward(grad_half, qkv_half, both_all, mixed):
            seq = lax.axis_size("seq")
            query_grad, both_grad = by_heads(
                patch_backward_kernel,
                (
                    jax.ShapeDtypeStruct((span_rows, width), half),
                    jax.ShapeDtypeStruct((seq, 2, span_rows, width), half),
                ),
                (
                    narrow_spec,
                    pl.BlockSpec((seq, 2, span_rows, LANES), lambda at: (0, 0, 0, at)),
                ),
                qkv_half,
                both_all,
                bias,
                grad_half,
            )
            pairs = both_grad.reshape(seq // 2, 2, 2, span_rows, width)
            core = lax.axis_index("seq") % 2
            got = swap(pick(pairs, 1 - core, 1), "seq", 1)
            key_value_grad = to_half(along_depth(wide(pick(pairs, core, 1)) + wide(got)))
            return jnp.concatenate([query_grad, key_value_grad[0], key_value_grad[1]], axis=1)

        byte_grid = my_bytes.reshape(span_rows, PATCH)
        resid = jnp.where(starts[:, None], vectors[5][None, :], projected)
        top, saved_top = layer_forward(
            resid, vectors[0:2], qkv_w[0], out_w[0], in_w[0], down_w[0], global_forward
        )
        top, active_blocks = lax.optimization_barrier((top, column_blocks(saved_top[11:])))
        (active_columns,) = deal_columns(active_blocks, saved_top[11:])
        patch_sides = gather_rows(
            jnp.concatenate([saved_top[2], saved_top[5], saved_top[9]], axis=1)
        )
        before = jnp.concatenate([jnp.zeros((span_rows, 1), jnp.int32), byte_grid[:, :-1]], axis=1)
        before_hot = one_hot(before, VOCAB, half)
        local_embed = jnp.dot(before_hot, table_w[1], preferred_element_type=single).reshape(
            span_rows, PATCH, width
        )
        local_in = (
            local_embed * keep_first[None, :, None] + top[:, None, :] + vectors[6 : 6 + PATCH][None]
        )
        result, saved_low = layer_forward(
            local_in.reshape(span_rows * PATCH, width),
            vectors[2:4],
            qkv_w[1],
            out_w[1],
            in_w[1],
            down_w[1],
            local_forward,
        )
        final, (final_normed, final_scale) = norm_forward(result, vectors[4])
        final_half = final.astype(half)
        logits = jnp.einsum("rd,vd->rv", final_half, table_w[2], preferred_element_type=single)
        shifted = logits - jnp.max(logits, axis=-1, keepdims=True)
        totals = jnp.sum(jnp.exp(shifted), axis=-1, keepdims=True)
        probs = jnp.exp(shifted) / totals
        target_hot = one_hot(my_bytes, VOCAB, single)
        losses = jnp.log(totals[:, 0]) - jnp.sum(shifted * target_hot, axis=-1)
        loss_terms = jnp.sum(losses[:, None] * group_hot, axis=0)
        row_weight = jnp.sum(group_hot * (1.0 / (GROUPS * counts))[None, :], axis=-1)
        logit_half = (row_weight[:, None] * (probs - target_hot)).astype(half)
        head_grad = jnp.einsum("rv,rd->vd", logit_half, final_half, preferred_element_type=single)
        final_grad = jnp.einsum("rv,vd->rd", logit_half, table_w[2], preferred_element_type=single)
        result_grad, final_gain_grad = norm_backward(
            final_grad, final_normed, final_scale, vectors[4]
        )
        running, sides = {}, {}

        def after_low(where, value, *others):
            if where == "mlp":
                grads = [to_half(outer(pair)) for pair in others]
                running["early"] = Stepped(group_steps(grads + [to_half(head_grad)], width))
            elif where == "attention":
                value, sides["active"] = lax.optimization_barrier((value, active_columns))
            elif where == "projections":
                attn_half, mixed_half, proj_half = others
                value, sides["all"] = lax.optimization_barrier((value, patch_sides))
                value, proj_half = advance([value, proj_half], running["early"])
                sides["qkv"], sides["out"] = (attn_half, value), (mixed_half, proj_half)
                return value
            (value,) = advance([value], running["early"])
            return value

        def after_top(where, value, *others):
            if where == "mlp":
                sides["mlp"] = others[0][1]
                (value,) = advance([value], running["low"])
            elif where == "attention":
                (value,) = advance([value], running["early"], running["low"])
            elif where == "projections":
                value, sides["top"] = lax.optimization_barrier((value, top_all))
                (value,) = tie([value], [running["low"]])
                sides["patch"] = [value, others[2], sides["mlp"]]
            return value

        local_grad, low_gains = layer_backward(
            result_grad,
            saved_low,
            vectors[2:4],
            qkv_w[1],
            out_w[1],
            in_w[1],
            down_w[1],
            local_backward,
            after_low,
        )
        grid_grad = local_grad.reshape(span_rows, PATCH, width)
        top_grad = jnp.sum(grid_grad, axis=1)
        position_grad = jnp.sum(grid_grad, axis=0)
        masked_grad = (grid_grad * keep_first[None, :, None]).reshape(span_rows * PATCH, width)
        local_table_grad = hot_sum(before_hot, masked_grad)
        top_all = gather_rows(to_half(top_grad))
        low_partials = [to_half(outer(sides["qkv"])), to_half(outer(sides["out"]))]
        running["low"] = Stepped(
            group_steps(low_partials + [to_half(local_table_grad)], width, deal=False)
        )
        (top_grad,) = advance([top_grad], running["low"])
        resid_grad, top_gains = layer_backward(
            top_grad,
            saved_top,
            vectors[0:2],
            qkv_w[0],
            out_w[0],
            in_w[0],
            down_w[0],
            global_backward,
            after_top,
        )
        start_grad = jnp.sum(jnp.where(starts[:, None], resid_grad, 0.0), axis=0)
        projected_half = jnp.where(starts[:, None], 0.0, resid_grad).astype(half)
        vector_grad = jnp.concatenate(
            [top_gains, low_gains, final_gain_grad[None], start_grad[None], position_grad],
            axis=0,
        )
        own = jnp.broadcast_to(
            projected_half[None], (lax.axis_size("seq") // 2,) + projected_half.shape
        )
        joint = deal_depth(jnp.concatenate([own, running["low"].held[0]], axis=1))
        joint, patch, patch_down = lax.optimization_barrier(
            (joint, column_blocks(sides["patch"]), outer((sides["active"], sides["top"])))
        )
        running["low"].feed([joint[:, span_rows:]])
        running["gather"] = Stepped(gather_steps(joint[:, :span_rows]))
        advance([], running["gather"])
        columns = deal_columns(patch, sides["patch"])
        advance([], running["gather"])
        advance([], running["gather"])
        attn_all, mixed_all, mlp_all = (
            sides["all"][:, at * width : (at + 1) * width] for at in range(3)
        )
        blocks = [outer(pair) for pair in zip((attn_all, mixed_all, mlp_all), columns)]
        dealt_rows = deal_rows(blocks)
        advance([], running["gather"])
        projected_all = running["gather"].result
        proj_grad = jnp.einsum(
            "ri,rd->id", embed_part, projected_all, preferred_element_type=single
        )
        embed_grad = jnp.einsum(
            "rd,id->ri", projected_all, proj_half, preferred_element_type=single
        )
        slot_grad = hot_sum(slot_hot, embed_grad)
        slot_grad, dealt_rows = lax.optimization_barrier((slot_grad, dealt_rows))
        patch_qkv, patch_out, patch_in = whole_rows(dealt_rows, blocks)
        slot_size, vector_rows = slot_grad.size // count, spread(vector_grad.reshape(-1))
        dealt = lax.all_to_all(
            jnp.concatenate([slot_grad.reshape(count, slot_size), vector_rows], axis=1),
            ("items", "seq"),
            0,
            0,
            tiled=True,
        )
        vector_piece = jnp.sum(dealt[:, slot_size:], axis=0)
        slot_rows = dealt[:, :slot_size].reshape(count, -1, mine)
        slot_rows = jnp.sum(slot_rows.reshape(PATCH, splits, -1, mine), axis=0)
        global_table_grad = slot_rows.transpose(1, 0, 2).reshape(-1, width)
        assert all(group.result is not None for group in running.values())
        early, low = running["early"].result, running["low"].result
        owned = (
            proj_grad,
            jnp.stack([global_table_grad, low[2], early[2]]),
            jnp.stack([patch_qkv, low[0]]),
            jnp.stack([patch_out, low[1]]),
            jnp.stack([patch_in, early[0]]),
            jnp.stack([patch_down, early[1]]),
        )
        pieces = [proj_grad, global_table_grad, *low, *early, patch_down, vector_piece]
        shard_square = sum(jnp.sum(piece * piece) for piece in pieces + [wide(dealt_rows)])
        return (loss_terms, owned, vector_piece, shard_square)

    loss_terms, owned, vector_piece, shard_square = item_pass(
        byte_tokens[0], groups[0], doc_ids[0]
    )
    tail = share(jnp.concatenate([vector_piece, shard_square[None], loss_terms]))
    size = vector_piece.shape[0]
    vector_total = tail[:, :size].reshape(-1)[: vectors.size].reshape(vectors.shape)
    loss_total = jnp.sum(tail[:, size + 1 :], axis=0)
    loss = jnp.sum(loss_total / counts) / GROUPS
    grad_norm = jnp.sqrt(jnp.sum(tail[:, size]))
    factor = jnp.minimum(1.0, CLIP_AT / grad_norm)
    step = float(STEP_NUMBER)
    rates = (
        (PATCH * D) ** (-0.5),
        jnp.array([1.0, 1.0, 2.0 * D ** (-0.5)], single).reshape(3, 1, 1),
        D ** (-0.5),
        (D // 8) ** (-0.5),
        D ** (-0.5),
        FF ** (-0.5),
        0.5,
    )
    masters = (patch_proj, tables, attn_qkv, attn_out, mlp_in, mlp_out, vectors)
    grads = tuple(owned) + (vector_total,)
    firsts = (first_proj, first_tables, first_qkv, first_out, first_in, first_down, first_vectors)
    seconds = (
        second_proj,
        second_tables,
        second_qkv,
        second_out,
        second_in,
        second_down,
        second_vectors,
    )
    done = [
        adam_step(masters[n], grads[n] * factor, firsts[n], seconds[n], rates[n], step)
        for n in range(7)
    ]
    return (
        loss,
        grad_norm,
        done[0][0],
        done[1][0],
        done[2][0],
        done[3][0],
        done[4][0],
        done[5][0],
        done[6][0],
        done[0][1],
        done[1][1],
        done[2][1],
        done[3][1],
        done[4][1],
        done[5][1],
        done[6][1],
        done[0][2],
        done[1][2],
        done[2][2],
        done[3][2],
        done[4][2],
        done[5][2],
        done[6][2],
    )


def solution(mesh):
    return jax.shard_map(
        body,
        mesh=mesh,
        in_specs=(
            P("items", "seq"),
            P("items", "seq"),
            P("items", None),
            P(("items", "seq"), None),
            P(None, ("items", "seq"), None),
            P(None, ("items", "seq"), None),
            P(None, ("items", "seq"), None),
            P(None, ("items", "seq"), None),
            P(None, ("items", "seq"), None),
            P(),
            P(("items", "seq"), None),
            P(None, ("items", "seq"), None),
            P(None, ("items", "seq"), None),
            P(None, ("items", "seq"), None),
            P(None, ("items", "seq"), None),
            P(None, ("items", "seq"), None),
            P(),
            P(("items", "seq"), None),
            P(None, ("items", "seq"), None),
            P(None, ("items", "seq"), None),
            P(None, ("items", "seq"), None),
            P(None, ("items", "seq"), None),
            P(None, ("items", "seq"), None),
            P(),
        ),
        out_specs=(
            P(),
            P(),
            P(("items", "seq"), None),
            P(None, ("items", "seq"), None),
            P(None, ("items", "seq"), None),
            P(None, ("items", "seq"), None),
            P(None, ("items", "seq"), None),
            P(None, ("items", "seq"), None),
            P(),
            P(("items", "seq"), None),
            P(None, ("items", "seq"), None),
            P(None, ("items", "seq"), None),
            P(None, ("items", "seq"), None),
            P(None, ("items", "seq"), None),
            P(None, ("items", "seq"), None),
            P(),
            P(("items", "seq"), None),
            P(None, ("items", "seq"), None),
            P(None, ("items", "seq"), None),
            P(None, ("items", "seq"), None),
            P(None, ("items", "seq"), None),
            P(None, ("items", "seq"), None),
            P(),
        ),
        check_vma=False,
    )
```

```python
import jax
import jax.numpy as jnp
from jax import lax
from jax.experimental import pallas as pl
from jax.experimental.pallas import tpu as pltpu
from jax.sharding import PartitionSpec as P

D = 768
HEAD_DIM = 64
FF = 3072
PATCH = 8
VOCAB = 256
GROUPS = 4
STEP_NUMBER = 7


EPSILON = 1e-05
CLIP_AT = 0.01
BETA_ONE = 0.9
BETA_TWO = 0.95
ADAM_EPS = 1e-08
DECAY = 0.1
NEGATIVE = -1e30


def norm_forward(values, gain):
    scale = lax.rsqrt(jnp.mean(values * values, axis=-1, keepdims=True) + EPSILON)
    normed = values * scale
    return (normed * gain, (normed, scale))


def norm_backward(upstream, normed, scale, gain):
    gain_grad = jnp.sum(upstream * normed, axis=0)
    inner = upstream * gain
    return (scale * (inner - normed * jnp.mean(inner * normed, axis=-1, keepdims=True)), gain_grad)


def to_half(value):
    return value.astype(jnp.bfloat16)


def wide(value):
    return value.astype(jnp.float32)


def pick(value, index, axis):
    return lax.dynamic_index_in_dim(value, index, axis, keepdims=False)


def swap(value, axis, bit):
    count = lax.axis_size(axis)
    return lax.ppermute(value, axis, [(at, at ^ bit) for at in range(count)])


def same_core():
    seq = lax.axis_size("seq")
    return [list(range(first, seq, 2)) for first in range(2)]


def deal_depth(value):
    return lax.all_to_all(
        to_half(value), "seq", 0, 0, axis_index_groups=same_core(), tiled=True
    )


def along_depth(value):
    return jnp.sum(wide(deal_depth(value)), axis=0)


def gather_seq(value):
    seq = lax.axis_size("seq")
    mine = lax.all_to_all(
        jnp.broadcast_to(value[None], (seq // 2,) + value.shape),
        "seq",
        0,
        0,
        axis_index_groups=same_core(),
        tiled=True,
    )
    other = swap(mine, "seq", 1)
    second = lax.axis_index("seq") % 2 == 1
    pair = jnp.stack([jnp.where(second, other, mine), jnp.where(second, mine, other)], axis=1)
    return pair.reshape(seq * value.shape[0], value.shape[1])


def group_steps(partials, width, deal=True):
    items, seq = lax.axis_size("items"), lax.axis_size("seq")
    at_item, at_seq = lax.axis_index("items"), lax.axis_index("seq")
    core, x_at, y_at = at_seq % 2, at_item % 2, at_item // 2
    depth = seq // 2
    grids = [
        part.reshape(items // 2, 2, depth, 2, part.shape[0] // (items * seq), part.shape[1])
        for part in partials
    ]

    def side(index):
        return jnp.concatenate(
            [
                pick(grid, index, 3)[..., begin : begin + width]
                for grid in grids
                for begin in range(0, grid.shape[-1], width)
            ],
            axis=3,
        )

    kept = side(core)
    (sent,) = yield (side(1 - core),)
    (got,) = yield (swap(sent, "seq", 1),)
    rows = kept.shape[3]
    cut = rows // 16 * 8
    halves = ((0, cut), (cut, rows))

    def cells(value, y_from, y_count, x_from, x_count, half):
        begin, end = halves[half]
        return lax.dynamic_slice(
            value,
            (y_from, x_from, 0, begin, 0),
            (y_count, x_count, depth, end - begin, width),
        )

    def pair_sum(*where):
        return wide(cells(kept, *where)) + wide(cells(got, *where))

    to_x, to_y = yield (
        to_half(pair_sum(0, 2, 1 - x_at, 1, 0)),
        to_half(pair_sum(1 - y_at, 1, 0, 2, 1)),
    )
    first_in, second_in = yield swap(to_x, "items", 1), swap(to_y, "items", 2)
    to_y, to_x = yield (
        to_half(
            pair_sum(1 - y_at, 1, x_at, 1, 0)
            + wide(lax.dynamic_slice_in_dim(first_in, 1 - y_at, 1, 0))
        ),
        to_half(
            pair_sum(y_at, 1, 1 - x_at, 1, 1)
            + wide(lax.dynamic_slice_in_dim(second_in, 1 - x_at, 1, 1))
        ),
    )
    first_end, second_end = yield swap(to_y, "items", 2), swap(to_x, "items", 1)
    first = (
        pair_sum(y_at, 1, x_at, 1, 0)
        + wide(lax.dynamic_slice_in_dim(first_in, y_at, 1, 0))
        + wide(first_end)
    )
    second = (
        pair_sum(y_at, 1, x_at, 1, 1)
        + wide(lax.dynamic_slice_in_dim(second_in, x_at, 1, 1))
        + wide(second_end)
    )
    (blocks,) = yield (
        jnp.concatenate([to_half(first[0, 0]), to_half(second[0, 0])], axis=1),
    )
    if deal:
        (blocks,) = yield (deal_depth(blocks),)
    rows = jnp.sum(wide(blocks), axis=0)
    out, at = [], 0
    for grid in grids:
        deep, pieces = grid.shape[4], []
        for _ in range(0, grid.shape[-1], width):
            pieces.append(rows[at : at + deep])
            at += deep
        out.append(jnp.concatenate(pieces, axis=1))
    return out


def in_order(mine, other, bit, axis):
    return jnp.stack(
        [jnp.where(bit == 1, other, mine), jnp.where(bit == 1, mine, other)], axis=axis
    )


def gather_steps(mine):
    items, seq = lax.axis_size("items"), lax.axis_size("seq")
    at_item, at_seq = lax.axis_index("items"), lax.axis_index("seq")
    core, x_at, y_at = at_seq % 2, at_item % 2, at_item // 2
    rows, width = mine.shape[1:]
    cut = width // 2
    first, second = yield (mine[..., :cut], mine[..., cut:])
    to_x, to_y = yield (swap(first, "items", 1), swap(second, "items", 2))
    first, second = yield (in_order(first, to_x, x_at, 0), in_order(second, to_y, y_at, 0))
    to_y, to_x = yield (swap(first, "items", 2), swap(second, "items", 1))
    (mine,) = yield (
        jnp.concatenate(
            [in_order(first, to_y, y_at, 0), in_order(second, to_x, x_at, 1)], axis=-1
        ),
    )
    (other,) = yield (swap(mine, "seq", 1),)
    return in_order(mine, other, core, 3).reshape(items * seq * rows, width)


class Stepped:
    def __init__(self, steps):
        self.steps = steps
        self.held = next(self.steps)
        self.sending = True
        self.result = None

    def feed(self, arrays):
        try:
            self.held = self.steps.send(tuple(arrays))
        except StopIteration as end:
            self.held, self.result = (), end.value
        self.sending = not self.sending


def tie(values, groups):
    flat = list(values)
    for group in groups:
        flat.extend(group.held)
    flat = list(lax.optimization_barrier(tuple(flat)))
    values, flat = flat[: len(values)], flat[len(values) :]
    for group in groups:
        size = len(group.held)
        group.feed(flat[:size])
        flat = flat[size:]
    return values


def advance(values, *groups):
    waiting = [group for group in groups if group.result is None and not group.sending]
    if waiting:
        values = tie(values, waiting)
    sending = [group for group in groups if group.result is None]
    return tie(values, sending) if sending else values


def reduce_group(partials, width):
    group = Stepped(group_steps(partials, width))
    while group.result is None:
        advance([], group)
    return group.result


def to_depth(value):
    half_seq = lax.axis_size("seq") // 2
    return deal_depth(jnp.broadcast_to(value[None], (half_seq,) + value.shape))


def gather_swaps(mine):
    group = Stepped(gather_steps(mine))
    while group.result is None:
        advance([], group)
    return group.result


def share(row):
    count = lax.axis_size("items") * lax.axis_size("seq")
    return lax.all_to_all(
        jnp.broadcast_to(row[None], (count,) + row.shape), ("items", "seq"), 0, 0, tiled=True
    )


def spread(value):
    count = lax.axis_size("items") * lax.axis_size("seq")
    size = -(-value.shape[0] // count)
    return jnp.pad(value, (0, size * count - value.shape[0])).reshape(count, size)


def square_row(piece, width):
    sums = jnp.sum(piece * piece, axis=0, keepdims=True)
    return sum(sums[:, at : at + width] for at in range(0, piece.shape[1], width))


def gather_rows(value):
    return lax.all_gather(value, ("items", "seq"), axis=0, tiled=True)


def one_hot(indices, width, dtype):
    return (indices.reshape(-1)[:, None] == jnp.arange(width)[None, :]).astype(dtype)


def hot_sum(hot, value):
    high = to_half(value)
    rest = to_half(value - wide(high))
    add = lambda term: jnp.einsum("rv,rd->vd", hot, term, preferred_element_type=jnp.float32)
    return add(high) + add(rest)


def layer_forward(resid, gains, qkv_w, out_w, in_w, down_w, attend):
    attn_in, (normed_one, scale_one) = norm_forward(resid, gains[0])
    attn_half = attn_in.astype(jnp.bfloat16)
    qkv_half = jnp.dot(attn_half, qkv_w, preferred_element_type=jnp.float32).astype(jnp.bfloat16)
    mixed, kept = attend(qkv_half)
    mixed_half = mixed.astype(jnp.bfloat16)
    middle = resid + jnp.dot(mixed_half, out_w, preferred_element_type=jnp.float32)
    mlp_norm, (normed_two, scale_two) = norm_forward(middle, gains[1])
    mlp_half = mlp_norm.astype(jnp.bfloat16)
    hidden = jnp.dot(mlp_half, in_w, preferred_element_type=jnp.float32)
    active_half = jax.nn.gelu(hidden).astype(jnp.bfloat16)
    result = middle + jnp.dot(active_half, down_w, preferred_element_type=jnp.float32)
    saved = (
        normed_one,
        scale_one,
        attn_half,
        qkv_half,
        mixed,
        mixed_half,
        kept,
        normed_two,
        scale_two,
        mlp_half,
        hidden,
        active_half,
    )
    return (result, saved)


def layer_backward(result_grad, saved, gains, qkv_w, out_w, in_w, down_w, attend_back, after):
    (
        normed_one,
        scale_one,
        attn_half,
        qkv_half,
        mixed,
        mixed_half,
        kept,
        normed_two,
        scale_two,
        mlp_half,
        hidden,
        active_half,
    ) = saved
    branch_half = result_grad.astype(jnp.bfloat16)
    active_grad = jnp.einsum("rd,fd->rf", branch_half, down_w, preferred_element_type=jnp.float32)
    _, gelu_back = jax.vjp(jax.nn.gelu, hidden)
    hidden_half = gelu_back(active_grad)[0].astype(jnp.bfloat16)
    hidden_half = after("mlp", hidden_half, (mlp_half, hidden_half), (active_half, branch_half))
    mlp_grad = jnp.einsum("rf,df->rd", hidden_half, in_w, preferred_element_type=jnp.float32)
    middle_grad, gain_two = norm_backward(mlp_grad, normed_two, scale_two, gains[1])
    middle_grad = middle_grad + result_grad
    proj_half = middle_grad.astype(jnp.bfloat16)
    mixed_grad = jnp.einsum("rd,ed->re", proj_half, out_w, preferred_element_type=jnp.float32)
    mixed_grad_half = after("attention", mixed_grad.astype(jnp.bfloat16))
    qkv_grad_half = attend_back(mixed_grad_half, qkv_half, kept, mixed).astype(jnp.bfloat16)
    qkv_grad_half = after("projections", qkv_grad_half, attn_half, mixed_half, proj_half)
    attn_grad = jnp.einsum("re,de->rd", qkv_grad_half, qkv_w, preferred_element_type=jnp.float32)
    resid_grad, gain_one = norm_backward(attn_grad, normed_one, scale_one, gains[0])
    resid_grad = after("end", resid_grad + middle_grad)
    return resid_grad, jnp.stack([gain_one, gain_two])


def outer(pair):
    return jnp.einsum("ri,rj->ij", *pair, preferred_element_type=jnp.float32)


def column_blocks(parts):
    count = lax.axis_size("items") * lax.axis_size("seq")
    rows = parts[0].shape[0]
    blocks = jnp.concatenate([part.reshape(rows, count, -1) for part in parts], axis=2)
    return blocks.transpose(1, 0, 2)


def deal_columns(blocks, parts):
    count, rows = blocks.shape[:2]
    dealt = lax.all_to_all(blocks, ("items", "seq"), 0, 0, tiled=True).reshape(count * rows, -1)
    out, at = [], 0
    for part in parts:
        size = part.shape[1] // count
        out.append(dealt[:, at : at + size])
        at += size
    return out


def deal_rows(parts):
    count = lax.axis_size("items") * lax.axis_size("seq")
    blocks = jnp.concatenate([to_half(part) for part in parts], axis=1)
    return lax.all_to_all(
        blocks.reshape(count, -1, blocks.shape[1]), ("items", "seq"), 0, 0, tiled=True
    )


def whole_rows(dealt, parts):
    out, at = [], 0
    for part in parts:
        size = part.shape[1]
        piece = dealt[:, :, at : at + size].transpose(1, 0, 2)
        out.append(wide(piece.reshape(piece.shape[0], -1)))
        at += size
    return out


ROWS = 128
LANES = 128


def contract(left, right, left_dim, right_dim):
    return lax.dot_general(
        left, right, (((left_dim,), (right_dim,)), ((), ())), preferred_element_type=jnp.float32
    )


def local_masks():
    row = lax.broadcasted_iota(jnp.int32, (ROWS, ROWS), 0)
    column = lax.broadcasted_iota(jnp.int32, (ROWS, ROWS), 1)
    allowed = (row // PATCH == column // PATCH) & (column <= row)
    lane = lax.broadcasted_iota(jnp.int32, (ROWS, LANES), 1)
    lanes = [
        jnp.where(lane // HEAD_DIM == head, 1.0, 0.0).astype(jnp.bfloat16)
        for head in range(LANES // HEAD_DIM)
    ]
    return allowed, lanes


def local_probs(query, key, allowed):
    scores = contract(query, key, 1, 1) * HEAD_DIM ** (-0.5)
    scores = jnp.where(allowed, scores, NEGATIVE)
    raised = jnp.exp(scores - jnp.max(scores, axis=-1, keepdims=True))
    return raised / jnp.sum(raised, axis=-1, keepdims=True)


def local_forward_kernel(qkv_ref, mixed_ref):
    width = mixed_ref.shape[1]
    allowed, lanes = local_masks()
    for begin in range(0, width, LANES):
        query, key, value = (
            qkv_ref[:, part * width + begin : part * width + begin + LANES] for part in range(3)
        )
        mixed = jnp.zeros((ROWS, LANES), jnp.float32)
        for mask in lanes:
            probs = local_probs(query * mask, key, allowed).astype(jnp.bfloat16)
            mixed = mixed + contract(probs, value * mask, 1, 0)
        mixed_ref[:, begin : begin + LANES] = mixed.astype(jnp.bfloat16)


def local_backward_kernel(qkv_ref, grad_ref, out_ref):
    width = grad_ref.shape[1]
    allowed, lanes = local_masks()
    scale = HEAD_DIM ** (-0.5)
    for begin in range(0, width, LANES):
        query, key, value = (
            qkv_ref[:, part * width + begin : part * width + begin + LANES] for part in range(3)
        )
        upstream = grad_ref[:, begin : begin + LANES]
        sums = [jnp.zeros((ROWS, LANES), jnp.float32) for _ in range(3)]
        for mask in lanes:
            head_query, head_upstream = query * mask, upstream * mask
            probs = local_probs(head_query, key, allowed)
            prob_grad = contract(head_upstream, value, 1, 1)
            inner = jnp.sum(prob_grad * probs, axis=-1, keepdims=True)
            score_half = (probs * (prob_grad - inner)).astype(jnp.bfloat16)
            sums[0] = sums[0] + contract(score_half, key * mask, 1, 0)
            sums[1] = sums[1] + contract(score_half, head_query, 0, 0)
            sums[2] = sums[2] + contract(probs.astype(jnp.bfloat16), head_upstream, 0, 0)
        for part, factor in enumerate((scale, scale, 1.0)):
            at = part * width + begin
            out_ref[:, at : at + LANES] = (sums[part] * factor).astype(jnp.bfloat16)


def by_rows(kernel, out_width, *operands):
    rows = operands[0].shape[0]
    moved = sum(value.size for value in operands) * 2 + rows * out_width * 2
    return pl.pallas_call(
        kernel,
        grid=(rows // ROWS,),
        in_specs=[pl.BlockSpec((ROWS, value.shape[1]), lambda at: (at, 0)) for value in operands],
        out_specs=pl.BlockSpec((ROWS, out_width), lambda at: (at, 0)),
        out_shape=jax.ShapeDtypeStruct((rows, out_width), jnp.bfloat16),
        cost_estimate=pl.CostEstimate(
            flops=rows * ROWS * out_width * 8, bytes_accessed=moved, transcendentals=rows * ROWS
        ),
    )(*operands)


def local_forward(qkv_half):
    return by_rows(local_forward_kernel, qkv_half.shape[1] // 3, qkv_half), None


def local_backward(grad_half, qkv_half, kept, mixed):
    return by_rows(local_backward_kernel, qkv_half.shape[1], qkv_half, grad_half)


def patch_probs(query, key, bias):
    scores = contract(query, key, 1, 1) * HEAD_DIM ** (-0.5) + bias
    raised = jnp.exp(scores - jnp.max(scores, axis=-1, keepdims=True))
    return raised / jnp.sum(raised, axis=-1, keepdims=True)


def head_lanes():
    lane = lax.broadcasted_iota(jnp.int32, (1, LANES), 1)
    return [
        jnp.where(lane // HEAD_DIM == head, 1.0, 0.0).astype(jnp.bfloat16)
        for head in range(LANES // HEAD_DIM)
    ]


def patch_forward_kernel(query_ref, key_ref, value_ref, bias_ref, mixed_ref):
    mixed = jnp.zeros(mixed_ref.shape, jnp.float32)
    for mask in head_lanes():
        probs = patch_probs(query_ref[...] * mask, key_ref[...], bias_ref[...])
        mixed = mixed + contract(probs.astype(jnp.bfloat16), value_ref[...] * mask, 1, 0)
    mixed_ref[...] = mixed.astype(jnp.bfloat16)


def patch_backward_kernel(query_ref, key_ref, value_ref, bias_ref, grad_ref, query_out, both_out):
    seq, _, span, _ = both_out.shape
    query_grad = jnp.zeros(query_out.shape, jnp.float32)
    key_grad = jnp.zeros(key_ref.shape, jnp.float32)
    value_grad = jnp.zeros(key_ref.shape, jnp.float32)
    for mask in head_lanes():
        query, upstream, key = query_ref[...] * mask, grad_ref[...] * mask, key_ref[...]
        probs = patch_probs(query, key, bias_ref[...])
        prob_grad = contract(upstream, value_ref[...], 1, 1)
        inner = jnp.sum(prob_grad * probs, axis=-1, keepdims=True)
        score_half = (probs * (prob_grad - inner)).astype(jnp.bfloat16)
        query_grad = query_grad + contract(score_half, key * mask, 1, 0)
        key_grad = key_grad + contract(score_half, query, 0, 0)
        value_grad = value_grad + contract(probs.astype(jnp.bfloat16), upstream, 0, 0)
    scale = HEAD_DIM ** (-0.5)
    query_out[...] = (query_grad * scale).astype(jnp.bfloat16)
    both_out[:, 0] = (key_grad * scale).astype(jnp.bfloat16).reshape(seq, span, LANES)
    both_out[:, 1] = value_grad.astype(jnp.bfloat16).reshape(seq, span, LANES)


def by_heads(kernel, out_shape, out_specs, qkv_half, both_all, bias, *others):
    rows, total, pairs = qkv_half.shape[0], both_all.shape[0], both_all.shape[1] // 2 // LANES
    columns = lambda count, shift: pl.BlockSpec((count, LANES), lambda at: (0, at + shift))
    return pl.pallas_call(
        kernel,
        grid=(pairs,),
        in_specs=[
            columns(rows, 0),
            columns(total, 0),
            columns(total, pairs),
            pl.BlockSpec((rows, total), lambda at: (0, 0)),
        ]
        + [columns(rows, 0) for _ in others],
        out_specs=out_specs,
        out_shape=out_shape,
    )(qkv_half, both_all, both_all, bias, *others)


def adam_step(weight, grad, first, second, rate, count):
    first = BETA_ONE * first + (1.0 - BETA_ONE) * grad
    second = BETA_TWO * second + (1.0 - BETA_TWO) * grad * grad
    first_hat = first / (1.0 - BETA_ONE**count)
    second_hat = second / (1.0 - BETA_TWO**count)
    return (
        weight - rate * (first_hat / (jnp.sqrt(second_hat) + ADAM_EPS) + DECAY * weight),
        first,
        second,
    )


def body(
    byte_tokens,
    groups,
    doc_ids,
    patch_proj,
    tables,
    attn_qkv,
    attn_out,
    mlp_in,
    mlp_out,
    vectors,
    first_proj,
    first_tables,
    first_qkv,
    first_out,
    first_in,
    first_down,
    first_vectors,
    second_proj,
    second_tables,
    second_qkv,
    second_out,
    second_in,
    second_down,
    second_vectors,
):
    half = jnp.bfloat16
    single = jnp.float32
    width = vectors.shape[1]
    depth = attn_qkv.shape[1]
    count = lax.axis_size("items") * lax.axis_size("seq")
    rank = lax.axis_index("items") * lax.axis_size("seq") + lax.axis_index("seq")
    mine = patch_proj.shape[0]
    splits = width // mine
    slot, column = rank // splits, rank % splits
    narrow = tables[0].astype(half).reshape(-1, splits, mine).transpose(1, 0, 2)
    narrow = jnp.tile(narrow.reshape(splits, -1), (count // splits, 1))
    own = jnp.concatenate([byte_tokens.reshape(-1), groups.reshape(-1)]).astype(half)
    patch_mine = to_depth(jnp.concatenate([attn_qkv[0], attn_out[0]], axis=1).astype(half))
    patch_mine, own = lax.optimization_barrier((patch_mine, own))
    dealt = lax.all_to_all(
        jnp.concatenate([narrow, jnp.broadcast_to(own[None], (count,) + own.shape)], axis=1),
        ("items", "seq"),
        0,
        0,
        tiled=True,
    )
    told = dealt[:, narrow.shape[1] :].astype(jnp.int32).reshape(count, 2, -1)
    narrow = dealt[:, : narrow.shape[1]].reshape(-1, mine)
    counts = jnp.sum(one_hot(told[:, 1], GROUPS, single), axis=0)

    def flat(value):
        return jnp.concatenate(
            [value[at : at + depth] for at in range(0, value.shape[0], depth)], axis=1
        ).astype(half)

    def tall(value):
        pieces = [value[:, at : at + width] for at in range(0, value.shape[1], width)]
        pieces = [piece.reshape(count, 1, depth, width) for piece in pieces]
        return jnp.concatenate(pieces, axis=1)

    def layer_parts(n):
        return [
            attn_qkv[n].astype(half),
            attn_out[n].astype(half),
            mlp_in[n].astype(half),
            flat(mlp_out[n]),
        ]

    sizes = [3 * width, width, mlp_in.shape[2], mlp_out.shape[1] // depth * width]

    def cut(joined, begin, lengths):
        pieces = []
        for length in lengths:
            pieces.append(joined[:, begin : begin + length])
            begin += length
        return pieces

    patch_parts, byte_parts = layer_parts(0), layer_parts(1)
    patch_all = gather_swaps(patch_mine)
    rest_all = gather_rows(
        jnp.concatenate(
            patch_parts[2:] + byte_parts + [flat(tables.reshape(-1, width))], axis=1
        )
    )
    rest = cut(rest_all, 0, sizes[2:] + sizes + [tables.shape[0] * tables.shape[1] // depth * width])
    weights = [cut(patch_all, 0, sizes[:2]) + rest[:2], rest[2:6]]
    for part in weights:
        part[3] = tall(part[3]).reshape(-1, width)
    qkv_w, out_w, in_w, down_w = ([weights[n][at] for n in range(2)] for at in range(4))
    table_rows = rest[6].reshape(count, tables.shape[0], -1, width)
    table_w = [table_rows[:, n].reshape(-1, width) for n in range(3)]

    all_grid = told[:, 0].reshape(byte_tokens.shape[0] * lax.axis_size("items"), -1, PATCH)
    ahead = jnp.concatenate([jnp.zeros_like(all_grid[:, :1]), all_grid[:, :-1]], axis=1)
    slot_hot = one_hot(pick(ahead, slot, 2), VOCAB, half)
    embed_part = to_half(jnp.dot(slot_hot, narrow, preferred_element_type=single))
    proj_half = patch_proj.astype(half)
    projected_part = jnp.dot(embed_part, proj_half, preferred_element_type=single)
    projected = reduce_group([to_half(projected_part)], width)[0]
    span_rows = byte_tokens.shape[1] // PATCH
    total_patches = doc_ids.shape[1]
    offset = lax.axis_index("seq") * span_rows
    my_pos = offset + jnp.arange(span_rows)
    keep_first = (jnp.arange(PATCH) > 0).astype(single)

    def item_pass(my_bytes, my_groups, all_docs):
        group_hot = one_hot(my_groups, GROUPS, single)
        my_docs = lax.dynamic_slice_in_dim(all_docs, offset, span_rows)
        prior_docs = jnp.concatenate(
            [lax.dynamic_slice_in_dim(all_docs, jnp.maximum(offset - 1, 0), 1), my_docs[:-1]]
        )
        starts = (my_pos == 0) | (my_docs != prior_docs)

        allowed = (jnp.arange(total_patches)[None, :] <= my_pos[:, None]) & (
            all_docs[None, :] == my_docs[:, None]
        )
        bias = jnp.where(allowed, 0.0, NEGATIVE)
        narrow_spec = pl.BlockSpec((span_rows, LANES), lambda at: (0, at))

        def global_forward(qkv_half):
            both_all = gather_seq(qkv_half[:, width:])
            mixed = by_heads(
                patch_forward_kernel,
                jax.ShapeDtypeStruct((span_rows, width), half),
                narrow_spec,
                qkv_half,
                both_all,
                bias,
            )
            return (mixed, both_all)

        def global_backward(grad_half, qkv_half, both_all, mixed):
            seq = lax.axis_size("seq")
            query_grad, both_grad = by_heads(
                patch_backward_kernel,
                (
                    jax.ShapeDtypeStruct((span_rows, width), half),
                    jax.ShapeDtypeStruct((seq, 2, span_rows, width), half),
                ),
                (
                    narrow_spec,
                    pl.BlockSpec((seq, 2, span_rows, LANES), lambda at: (0, 0, 0, at)),
                ),
                qkv_half,
                both_all,
                bias,
                grad_half,
            )
            pairs = both_grad.reshape(seq // 2, 2, 2, span_rows, width)
            core = lax.axis_index("seq") % 2
            got = swap(pick(pairs, 1 - core, 1), "seq", 1)
            key_value_grad = to_half(along_depth(wide(pick(pairs, core, 1)) + wide(got)))
            return jnp.concatenate([query_grad, key_value_grad[0], key_value_grad[1]], axis=1)

        byte_grid = my_bytes.reshape(span_rows, PATCH)
        resid = jnp.where(starts[:, None], vectors[5][None, :], projected)
        top, saved_top = layer_forward(
            resid, vectors[0:2], qkv_w[0], out_w[0], in_w[0], down_w[0], global_forward
        )
        top, active_blocks = lax.optimization_barrier((top, column_blocks(saved_top[11:])))
        (active_columns,) = deal_columns(active_blocks, saved_top[11:])
        patch_sides = gather_rows(
            jnp.concatenate([saved_top[2], saved_top[5], saved_top[9]], axis=1)
        )
        before = jnp.concatenate([jnp.zeros((span_rows, 1), jnp.int32), byte_grid[:, :-1]], axis=1)
        before_hot = one_hot(before, VOCAB, half)
        local_embed = jnp.dot(before_hot, table_w[1], preferred_element_type=single).reshape(
            span_rows, PATCH, width
        )
        local_in = (
            local_embed * keep_first[None, :, None] + top[:, None, :] + vectors[6 : 6 + PATCH][None]
        )
        result, saved_low = layer_forward(
            local_in.reshape(span_rows * PATCH, width),
            vectors[2:4],
            qkv_w[1],
            out_w[1],
            in_w[1],
            down_w[1],
            local_forward,
        )
        final, (final_normed, final_scale) = norm_forward(result, vectors[4])
        final_half = final.astype(half)
        logits = jnp.einsum("rd,vd->rv", final_half, table_w[2], preferred_element_type=single)
        shifted = logits - jnp.max(logits, axis=-1, keepdims=True)
        totals = jnp.sum(jnp.exp(shifted), axis=-1, keepdims=True)
        probs = jnp.exp(shifted) / totals
        target_hot = one_hot(my_bytes, VOCAB, single)
        losses = jnp.log(totals[:, 0]) - jnp.sum(shifted * target_hot, axis=-1)
        loss_terms = jnp.sum(losses[:, None] * group_hot, axis=0)
        row_weight = jnp.sum(group_hot * (1.0 / (GROUPS * counts))[None, :], axis=-1)
        logit_half = (row_weight[:, None] * (probs - target_hot)).astype(half)
        head_grad = jnp.einsum("rv,rd->vd", logit_half, final_half, preferred_element_type=single)
        final_grad = jnp.einsum("rv,vd->rd", logit_half, table_w[2], preferred_element_type=single)
        result_grad, final_gain_grad = norm_backward(
            final_grad, final_normed, final_scale, vectors[4]
        )
        running, sides = {}, {}

        def after_low(where, value, *others):
            if where == "mlp":
                grads = [to_half(outer(pair)) for pair in others]
                running["early"] = Stepped(group_steps(grads + [to_half(head_grad)], width))
            elif where == "attention":
                value, sides["active"] = lax.optimization_barrier((value, active_columns))
            elif where == "projections":
                attn_half, mixed_half, proj_half = others
                value, sides["all"] = lax.optimization_barrier((value, patch_sides))
                value, proj_half = advance([value, proj_half], running["early"])
                sides["qkv"], sides["out"] = (attn_half, value), (mixed_half, proj_half)
                return value
            (value,) = advance([value], running["early"])
            return value

        def after_top(where, value, *others):
            if where == "mlp":
                sides["mlp"] = others[0][1]
                (value,) = advance([value], running["low"])
            elif where == "attention":
                (value,) = advance([value], running["early"], running["low"])
            elif where == "projections":
                value, sides["top"] = lax.optimization_barrier((value, top_all))
                (value,) = tie([value], [running["low"]])
                sides["patch"] = [value, others[2], sides["mlp"]]
            return value

        local_grad, low_gains = layer_backward(
            result_grad,
            saved_low,
            vectors[2:4],
            qkv_w[1],
            out_w[1],
            in_w[1],
            down_w[1],
            local_backward,
            after_low,
        )
        grid_grad = local_grad.reshape(span_rows, PATCH, width)
        top_grad = jnp.sum(grid_grad, axis=1)
        position_grad = jnp.sum(grid_grad, axis=0)
        masked_grad = (grid_grad * keep_first[None, :, None]).reshape(span_rows * PATCH, width)
        local_table_grad = hot_sum(before_hot, masked_grad)
        top_all = gather_rows(to_half(top_grad))
        low_partials = [to_half(outer(sides["qkv"])), to_half(outer(sides["out"]))]
        running["low"] = Stepped(
            group_steps(low_partials + [to_half(local_table_grad)], width, deal=False)
        )
        (top_grad,) = advance([top_grad], running["low"])
        resid_grad, top_gains = layer_backward(
            top_grad,
            saved_top,
            vectors[0:2],
            qkv_w[0],
            out_w[0],
            in_w[0],
            down_w[0],
            global_backward,
            after_top,
        )
        start_grad = jnp.sum(jnp.where(starts[:, None], resid_grad, 0.0), axis=0)
        projected_half = jnp.where(starts[:, None], 0.0, resid_grad).astype(half)
        vector_grad = jnp.concatenate(
            [top_gains, low_gains, final_gain_grad[None], start_grad[None], position_grad],
            axis=0,
        )
        own = jnp.broadcast_to(
            projected_half[None], (lax.axis_size("seq") // 2,) + projected_half.shape
        )
        joint = deal_depth(jnp.concatenate([own, running["low"].held[0]], axis=1))
        joint, patch, patch_down = lax.optimization_barrier(
            (joint, column_blocks(sides["patch"]), outer((sides["active"], sides["top"])))
        )
        running["low"].feed([joint[:, span_rows:]])
        running["gather"] = Stepped(gather_steps(joint[:, :span_rows]))
        advance([], running["gather"])
        columns = deal_columns(patch, sides["patch"])
        advance([], running["gather"])
        advance([], running["gather"])
        attn_all, mixed_all, mlp_all = (
            sides["all"][:, at * width : (at + 1) * width] for at in range(3)
        )
        blocks = [outer(pair) for pair in zip((attn_all, mixed_all, mlp_all), columns)]
        dealt_rows = deal_rows(blocks)
        advance([], running["gather"])
        projected_all = running["gather"].result
        proj_grad = jnp.einsum(
            "ri,rd->id", embed_part, projected_all, preferred_element_type=single
        )
        embed_grad = jnp.einsum(
            "rd,id->ri", projected_all, proj_half, preferred_element_type=single
        )
        slot_grad = hot_sum(slot_hot, embed_grad)
        slot_size, vector_rows = slot_grad.size // count, spread(vector_grad.reshape(-1))
        own = [
            slot_grad.reshape(count, slot_size),
            vector_rows,
            jnp.broadcast_to(loss_terms[None], (count, GROUPS)),
        ]
        own, dealt_rows = lax.optimization_barrier((jnp.concatenate(own, axis=1), dealt_rows))
        dealt = lax.all_to_all(own, ("items", "seq"), 0, 0, tiled=True)
        vector_piece = jnp.sum(dealt[:, slot_size:-GROUPS], axis=0)
        loss_total = jnp.sum(dealt[:, -GROUPS:], axis=0)
        slot_rows = dealt[:, :slot_size].reshape(count, -1, mine)
        slot_rows = jnp.sum(slot_rows.reshape(PATCH, splits, -1, mine), axis=0)
        global_table_grad = slot_rows.transpose(1, 0, 2).reshape(-1, width)
        assert all(group.result is not None for group in running.values())
        early, low = running["early"].result, running["low"].result
        pieces = [*low, *early, patch_down, proj_grad, global_table_grad]
        squares = sum(square_row(piece, width) for piece in pieces)
        dealt_squares = jnp.sum(wide(dealt_rows) * wide(dealt_rows), axis=(0, 1))
        row = jnp.concatenate([vector_piece, squares[0], dealt_squares])
        row, dealt_rows = lax.optimization_barrier((row, dealt_rows))
        tail = share(row)
        patch_qkv, patch_out, patch_in = whole_rows(dealt_rows, blocks)
        owned = (
            proj_grad,
            jnp.stack([global_table_grad, low[2], early[2]]),
            jnp.stack([patch_qkv, low[0]]),
            jnp.stack([patch_out, low[1]]),
            jnp.stack([patch_in, early[0]]),
            jnp.stack([patch_down, early[1]]),
        )
        return (loss_total, owned, tail, vector_piece.shape[0])

    loss_total, owned, tail, size = item_pass(byte_tokens[0], groups[0], doc_ids[0])
    vector_total = tail[:, :size].reshape(-1)[: vectors.size].reshape(vectors.shape)
    loss = jnp.sum(loss_total / counts) / GROUPS
    grad_norm = jnp.sqrt(jnp.sum(tail[:, :size] * tail[:, :size]) + jnp.sum(tail[:, size:]))
    factor = jnp.minimum(1.0, CLIP_AT / grad_norm)
    step = float(STEP_NUMBER)
    rates = (
        (PATCH * D) ** (-0.5),
        jnp.array([1.0, 1.0, 2.0 * D ** (-0.5)], single).reshape(3, 1, 1),
        D ** (-0.5),
        (D // 8) ** (-0.5),
        D ** (-0.5),
        FF ** (-0.5),
        0.5,
    )
    masters = (patch_proj, tables, attn_qkv, attn_out, mlp_in, mlp_out, vectors)
    grads = tuple(owned) + (vector_total,)
    firsts = (first_proj, first_tables, first_qkv, first_out, first_in, first_down, first_vectors)
    seconds = (
        second_proj,
        second_tables,
        second_qkv,
        second_out,
        second_in,
        second_down,
        second_vectors,
    )
    done = [
        adam_step(masters[n], grads[n] * factor, firsts[n], seconds[n], rates[n], step)
        for n in range(7)
    ]
    return (
        loss,
        grad_norm,
        done[0][0],
        done[1][0],
        done[2][0],
        done[3][0],
        done[4][0],
        done[5][0],
        done[6][0],
        done[0][1],
        done[1][1],
        done[2][1],
        done[3][1],
        done[4][1],
        done[5][1],
        done[6][1],
        done[0][2],
        done[1][2],
        done[2][2],
        done[3][2],
        done[4][2],
        done[5][2],
        done[6][2],
    )


def solution(mesh):
    return jax.shard_map(
        body,
        mesh=mesh,
        in_specs=(
            P("items", "seq"),
            P("items", "seq"),
            P("items", None),
            P(("items", "seq"), None),
            P(None, ("items", "seq"), None),
            P(None, ("items", "seq"), None),
            P(None, ("items", "seq"), None),
            P(None, ("items", "seq"), None),
            P(None, ("items", "seq"), None),
            P(),
            P(("items", "seq"), None),
            P(None, ("items", "seq"), None),
            P(None, ("items", "seq"), None),
            P(None, ("items", "seq"), None),
            P(None, ("items", "seq"), None),
            P(None, ("items", "seq"), None),
            P(),
            P(("items", "seq"), None),
            P(None, ("items", "seq"), None),
            P(None, ("items", "seq"), None),
            P(None, ("items", "seq"), None),
            P(None, ("items", "seq"), None),
            P(None, ("items", "seq"), None),
            P(),
        ),
        out_specs=(
            P(),
            P(),
            P(("items", "seq"), None),
            P(None, ("items", "seq"), None),
            P(None, ("items", "seq"), None),
            P(None, ("items", "seq"), None),
            P(None, ("items", "seq"), None),
            P(None, ("items", "seq"), None),
            P(),
            P(("items", "seq"), None),
            P(None, ("items", "seq"), None),
            P(None, ("items", "seq"), None),
            P(None, ("items", "seq"), None),
            P(None, ("items", "seq"), None),
            P(None, ("items", "seq"), None),
            P(),
            P(("items", "seq"), None),
            P(None, ("items", "seq"), None),
            P(None, ("items", "seq"), None),
            P(None, ("items", "seq"), None),
            P(None, ("items", "seq"), None),
            P(None, ("items", "seq"), None),
            P(),
        ),
        check_vma=False,
    )
```
